8 devices in a mesh: dp: 1 (over z), tp: 2 (over y), kvp: 4 (over x, core).
Axes of the slice: x: 2, y: 2, z: 1, core: 2. Of those that a mesh axis runs over, the one named last changes fastest.
Arguments:
- x_in: bfloat16 [32, 5120], P('dp')
- ctx_len: int32 [32], P('dp')
- g_attn: bfloat16 [5120], replicated
- g_mlp: bfloat16 [5120], replicated
- w_qkv: bfloat16 [5120, 7168], P(None, 'tp')
- w_o: bfloat16 [5120, 5120], P(('tp', 'kvp'))
- w_gate: bfloat16 [5120, 13824], P(None, ('tp', 'kvp'))
- w_up: bfloat16 [5120, 13824], P(None, ('tp', 'kvp'))
- w_down: bfloat16 [13824, 5120], P(('tp', 'kvp'))
- k_cache: bfloat16 [32, 1024, 8, 128], P('dp', 'kvp', 'tp')
- v_cache: bfloat16 [32, 1024, 8, 128], P('dp', 'kvp', 'tp')
Outputs:
- output 1: bfloat16 [32, 5120], P('dp')
- output 2: bfloat16 [32, 1024, 8, 128], P('dp', 'kvp', 'tp')
- output 3: bfloat16 [32, 1024, 8, 128], P('dp', 'kvp', 'tp')
All inputs are finite; a program needn't handle non-finite values.
Results may differ from the reference program's by a relative error of at most 0.00830868.
Values sent between devices are 32-bit elements.
A program may use at most 1 GiB of HBM per device.

```python
import jax
import jax.numpy as jnp
from jax import lax

D = 5120
HEADS = 40
KV_HEADS = 8
HEAD = 128
FF = 13824
BATCH = 32
SEQ = 1024
NSEG = 16
GROUP = HEADS // KV_HEADS
ROPE_THETA = 500000.0
EPS = 1e-5
NEG_FILL = -1e30


def rms_norm(values, gain_vec):
    x_f32 = values.astype(jnp.float32)
    inv_rms = lax.rsqrt(jnp.mean(x_f32 * x_f32, axis=-1, keepdims=True) + EPS)
    return (x_f32 * inv_rms * gain_vec.astype(jnp.float32)).astype(jnp.bfloat16)


def rope_tables(ctx_len):
    inv_freq = ROPE_THETA ** (-2.0 * jnp.arange(HEAD // 2, dtype=jnp.float32) / HEAD)
    angles = ctx_len.astype(jnp.float32)[:, None] * inv_freq[None, :]
    return jnp.cos(angles), jnp.sin(angles)


def rotary(vectors, cos_t, sin_t):
    half_dim = vectors.shape[-1] // 2
    first_half = vectors[..., :half_dim]
    second_half = vectors[..., half_dim:]
    return jnp.concatenate([first_half * cos_t - second_half * sin_t, second_half * cos_t + first_half * sin_t], axis=-1)


def setup_inputs(seed: int = 0, part: int = 0) -> dict:
    root_key = jax.random.key(seed)
    shared_keys = jax.random.split(root_key, 7)
    part_keys = jax.random.split(jax.random.fold_in(root_key, part), 7)
    x_in = jax.random.normal(part_keys[0], (BATCH, D), jnp.float32).astype(jnp.bfloat16)
    ctx_len = jax.random.randint(part_keys[1], (BATCH,), SEQ // 4, SEQ, dtype=jnp.int32)
    full_row = jax.random.randint(part_keys[2], (), 0, BATCH, dtype=jnp.int32)
    ctx_len = jnp.where(jnp.arange(BATCH) == full_row, SEQ - 1, ctx_len).astype(jnp.int32)
    g_attn = (1.0 + 0.3 * jax.random.normal(shared_keys[0], (D,), jnp.float32)).astype(jnp.bfloat16)
    g_mlp = (1.0 + 0.3 * jax.random.normal(shared_keys[1], (D,), jnp.float32)).astype(jnp.bfloat16)
    w_qkv = (jax.random.normal(shared_keys[2], (D, KV_HEADS * (GROUP + 2) * HEAD), jnp.float32) * D ** -0.5).astype(jnp.bfloat16)
    w_o = (jax.random.normal(shared_keys[3], (HEADS * HEAD, D), jnp.float32) * (HEADS * HEAD) ** -0.5).astype(jnp.bfloat16)
    w_gate = (jax.random.normal(shared_keys[4], (D, FF), jnp.float32) * D ** -0.5).astype(jnp.bfloat16)
    w_up = (jax.random.normal(shared_keys[5], (D, FF), jnp.float32) * D ** -0.5).astype(jnp.bfloat16)
    w_down = (jax.random.normal(shared_keys[6], (FF, D), jnp.float32) * FF ** -0.5).astype(jnp.bfloat16)
    seg_shape = (BATCH, NSEG, 1, KV_HEADS, HEAD)
    noise_shape = (BATCH, NSEG, SEQ // NSEG, KV_HEADS, HEAD)
    cache_shape = (BATCH, SEQ, KV_HEADS, HEAD)
    k_cache = (jax.random.normal(part_keys[3], noise_shape, jnp.float32) + 0.5 * jax.random.normal(part_keys[4], seg_shape, jnp.float32)).reshape(cache_shape).astype(jnp.bfloat16)
    v_cache = (0.5 * jax.random.normal(part_keys[5], noise_shape, jnp.float32) + 2.0 * jax.random.normal(part_keys[6], seg_shape, jnp.float32)).reshape(cache_shape).astype(jnp.bfloat16)
    return {"x_in": x_in, "ctx_len": ctx_len, "g_attn": g_attn, "g_mlp": g_mlp, "w_qkv": w_qkv, "w_o": w_o, "w_gate": w_gate, "w_up": w_up, "w_down": w_down, "k_cache": k_cache, "v_cache": v_cache}


def reference(x_in, ctx_len, g_attn, g_mlp, w_qkv, w_o, w_gate, w_up, w_down, k_cache, v_cache):
    normed = rms_norm(x_in, g_attn)
    qkv_all = jnp.dot(normed, w_qkv, preferred_element_type=jnp.float32).reshape(BATCH, KV_HEADS, GROUP + 2, HEAD)
    cos_t, sin_t = rope_tables(ctx_len)
    queries = rotary(qkv_all[:, :, :GROUP], cos_t[:, None, None, :], sin_t[:, None, None, :]).astype(jnp.bfloat16)
    key_new = rotary(qkv_all[:, :, GROUP], cos_t[:, None, :], sin_t[:, None, :]).astype(jnp.bfloat16)
    val_new = qkv_all[:, :, GROUP + 1].astype(jnp.bfloat16)
    positions = jnp.arange(SEQ)
    hit_mask = (positions[None, :] == ctx_len[:, None])[:, :, None, None]
    k_out = jnp.where(hit_mask, key_new[:, None], k_cache)
    v_out = jnp.where(hit_mask, val_new[:, None], v_cache)
    score_scale = HEAD ** -0.5

    def one_request(row_args):
        q_row, k_row, v_row, length = row_args
        scores = jnp.einsum("grd,tgd->grt", q_row.astype(jnp.float32), k_row.astype(jnp.float32)) * score_scale
        scores = jnp.where(positions <= length, scores, NEG_FILL)
        row_max = jnp.max(scores, axis=-1, keepdims=True)
        prob_w = jnp.exp(scores - row_max)
        denom_sum = jnp.sum(prob_w, axis=-1)
        numer_acc = jnp.einsum("grt,tgd->grd", prob_w.astype(jnp.bfloat16).astype(jnp.float32), v_row.astype(jnp.float32))
        return (numer_acc / denom_sum[..., None]).reshape(HEADS * HEAD)

    attn_all = lax.map(one_request, (queries, k_out, v_out, ctx_len)).astype(jnp.bfloat16)
    hidden = (x_in.astype(jnp.float32) + jnp.dot(attn_all, w_o, preferred_element_type=jnp.float32)).astype(jnp.bfloat16)
    normed_mlp = rms_norm(hidden, g_mlp)
    gate_pre = jnp.dot(normed_mlp, w_gate, preferred_element_type=jnp.float32)
    up_proj = jnp.dot(normed_mlp, w_up, preferred_element_type=jnp.float32)
    act_out = (jax.nn.silu(gate_pre) * up_proj).astype(jnp.bfloat16)
    x_out = (hidden.astype(jnp.float32) + jnp.dot(act_out, w_down, preferred_element_type=jnp.float32)).astype(jnp.bfloat16)
    return (x_out, k_out, v_out)
```

```python
import jax
import jax.numpy as jnp
from jax import lax
from jax.experimental import pallas as pl
from jax.experimental.pallas import tpu as pltpu
from jax.sharding import PartitionSpec as P

ROPE_THETA = 500000.0
EPS = 1e-5
NEG_FILL = -1e30
MESH = pl.DeviceIdType.MESH
F32 = jnp.float32
BF16 = jnp.bfloat16

D = 5120
HD = 128
B = 32
T = 256
KVL = 4
GRP = 5
ROWS = 24
QCOLS = (GRP + 2) * HD
FFL = 1728
VMEM_MAX = 67043328


def remote(src, dst, send, recv, dev):
    return pltpu.make_async_remote_copy(src_ref=src, dst_ref=dst, send_sem=send, recv_sem=recv, device_id=dev, device_id_type=MESH)


def enter(peers):
    barrier = pltpu.get_barrier_semaphore()
    for peer in peers:
        pl.semaphore_signal(barrier, inc=1, device_id=peer, device_id_type=MESH)
    pl.semaphore_wait(barrier, len(peers))


CHUNKS = ((0, 2), (2, 2), (4, 2), (6, 1))


def qkv_kernel(x_ref, g_ref, cos_ref, sin_ref, w_ref, q_ref, kn_ref, vn_ref, wbuf, u_ref, ex, w_sem, m_send, m_recv, x_send, x_recv, r_send, r_recv):
    j = lax.axis_index("kvp")
    mate = {"kvp": j + 1 - 2 * lax.rem(j, 2)}
    side = {"kvp": lax.rem(j + 2, 4)}

    def load(i):
        first, n = CHUNKS[i]
        cols = pl.ds(pl.multiple_of(j * QCOLS + first * HD, HD), n * HD)
        return pltpu.make_async_copy(w_ref.at[:, cols], wbuf.at[:, pl.ds(first * HD, n * HD)], w_sem.at[i])

    load(0).start()
    load(1).start()
    enter((mate, side))
    xf = x_ref[...].astype(F32)
    inv = lax.rsqrt(jnp.mean(xf * xf, axis=-1, keepdims=True) + EPS)
    u_ref[...] = (x_ref[...].astype(F32) * inv * g_ref[...].astype(F32)).astype(BF16)
    q_ref[...] = jnp.zeros_like(q_ref)

    def piece(slot, i):
        first, n = CHUNKS[i]
        return ex.at[slot, pl.ds(first, n)]

    def to_mate(i):
        return remote(piece(j, i), piece(j, i), m_send.at[i], m_recv.at[i], mate)

    def to_side(i):
        return remote(piece(j, i), piece(j, i), x_send.at[i], x_recv.at[i], side)

    def relay(i):
        slot = lax.rem(j + 2, 4)
        return remote(piece(slot, i), piece(slot, i), r_send.at[i], r_recv.at[i], mate)

    for i, (first, n) in enumerate(CHUNKS):
        load(i).wait()
        if i + 2 < len(CHUNKS):
            load(i + 2).start()
        res = jnp.dot(u_ref[...], wbuf[:, first * HD:(first + n) * HD], preferred_element_type=F32)
        for h in range(n):
            tile = res[:, h * HD:(h + 1) * HD]
            if first + h < GRP + 1:
                tile = tile * cos_ref[...] + pltpu.roll(tile, HD // 2, 1) * sin_ref[...]
            ex[j, first + h] = tile
        to_side(i).start()
        to_mate(i).start()
    for i in range(len(CHUNKS)):
        to_side(i).wait_recv()
        relay(i).start()
    for i in range(len(CHUNKS)):
        to_mate(i).wait_recv()
        relay(i).wait_recv()
    for g in range(KVL):
        for r in range(GRP):
            q_ref[pl.ds(g * GRP + r, B, stride=ROWS), :] = ex[g, r]
        kn = ex[g, GRP]
        vn = ex[g, GRP + 1]
        for half in range(2):
            kn_ref[pl.ds(half * KVL + g, B, stride=8), :] = kn
            vn_ref[pl.ds(half * KVL + g, B, stride=8), :] = vn
    for i in range(len(CHUNKS)):
        to_side(i).wait_send()
        to_mate(i).wait_send()
        relay(i).wait_send()


PAIRS = B // 2


def attn_kernel(ctx_ref, q_ref, kn_ref, vn_ref, k_ref, v_ref, part_ref, ko_ref, vo_ref, kbuf, vbuf, bias, acc2, m2, l2, in_sem, out_sem):
    base = lax.axis_index("kvp") * T

    def fetch(p, which):
        src, dst = ((k_ref, kbuf), (v_ref, vbuf))[which]
        return pltpu.make_async_copy(src.at[pl.ds(2 * p, 2)], dst.at[pl.ds(2 * p, 2)], in_sem.at[which, p])

    def flush(p, which):
        src, dst = ((kbuf, ko_ref), (vbuf, vo_ref))[which]
        return pltpu.make_async_copy(src.at[pl.ds(2 * p, 2)], dst.at[pl.ds(2 * p, 2)], out_sem.at[which, p])

    @pl.loop(0, PAIRS)
    def _(p):
        fetch(p, 0).start()
        fetch(p, 1).start()

    row = lax.broadcasted_iota(jnp.int32, (2 * ROWS, KVL * T), 0)
    row = jnp.where(row >= ROWS, row - ROWS, row)
    col = lax.broadcasted_iota(jnp.int32, (2 * ROWS, KVL * T), 1)
    head = (row >= GRP).astype(jnp.int32) + (row >= 2 * GRP).astype(jnp.int32) + (row >= 3 * GRP).astype(jnp.int32)
    bias[...] = jnp.where(head == (col & (KVL - 1)), 0.0, NEG_FILL)
    first_half = lax.broadcasted_iota(jnp.int32, (2 * ROWS, 1), 0) < ROWS
    wrow = lax.broadcasted_iota(jnp.int32, (16, HD), 0)

    def patch(b):
        pos = ctx_ref[b] - base

        @pl.when((pos >= 0) & (pos < T))
        def _():
            win = pl.ds(pl.multiple_of((pos // 4) * 16, 16), 16)
            hit = (wrow // KVL) == (pos & 3)
            for new_ref, buf in ((kn_ref, kbuf), (vn_ref, vbuf)):
                new8 = new_ref[pl.ds(b * 8, 8), :]
                new16 = jnp.concatenate([new8, new8], axis=0)
                buf[b, win, :] = jnp.where(hit, new16, buf[b, win, :].astype(F32)).astype(BF16)

    def attend(p):
        b = 2 * p
        q = q_ref[pl.ds(p * 2 * ROWS, 2 * ROWS), :]
        lhs = jnp.concatenate([jnp.where(first_half, q, 0.0), jnp.where(first_half, 0.0, q)], axis=1).astype(BF16)
        keys = jnp.concatenate([kbuf[b], kbuf[b + 1]], axis=1)
        s = lax.dot_general(lhs, keys, (((1,), (1,)), ((), ())), preferred_element_type=F32)
        lim = jnp.where(first_half, (ctx_ref[b] - base + 1) * KVL, (ctx_ref[b + 1] - base + 1) * KVL)
        cols = lax.broadcasted_iota(jnp.int32, (2 * ROWS, KVL * T), 1)
        s = jnp.where(cols < lim, s * HD ** -0.5 + bias[...], NEG_FILL)
        m = jnp.max(s, axis=1, keepdims=True)
        w = jnp.exp(s - m)
        values = jnp.concatenate([vbuf[b], vbuf[b + 1]], axis=1)
        o = jnp.dot(w.astype(BF16), values, preferred_element_type=F32)
        rows = pl.ds(p * 2 * ROWS, 2 * ROWS)
        acc2[rows, :] = jnp.where(first_half, o[:, :HD], o[:, HD:])
        m2[rows, :] = jnp.broadcast_to(m, (2 * ROWS, HD))
        l2[rows, :] = jnp.broadcast_to(jnp.sum(w, axis=1, keepdims=True), (2 * ROWS, HD))

    @pl.loop(0, PAIRS // 2)
    def _(it):
        for k in range(2):
            p = it * 2 + k
            fetch(p, 0).wait()
            fetch(p, 1).wait()
            patch(2 * p)
            patch(2 * p + 1)
            flush(p, 0).start()
            flush(p, 1).start()
        for k in range(2):
            attend(it * 2 + k)

    lane = lax.broadcasted_iota(jnp.int32, (B, HD), 1)
    for g in range(KVL):
        stats = jnp.zeros((B, HD), F32)
        for r in range(GRP):
            rows = pl.ds(g * GRP + r, B, stride=ROWS)
            part_ref[g, r] = acc2[rows, :]
            stats = jnp.where(lane == r, m2[rows, :], stats)
            stats = jnp.where(lane == 8 + r, l2[rows, :], stats)
        part_ref[g, GRP] = stats

    @pl.loop(0, PAIRS)
    def _(p):
        flush(p, 0).wait()
        flush(p, 1).wait()


NCH = 5
CW = D // NCH
GCH = 256


def tail_kernel(part_ref, x_ref, g_ref, wo_hbm, wg_hbm, wu_hbm, wd_hbm, out_ref,
                wo, wg, wu, wd, rx, attn, n_ref, y_ref, pbuf, sbuf, pair_a, pair_b, rs_a, rs_b, ag_a, ag_b,
                w_sem, gu_sem, wd_sem, c_send, c_recv, d_send, d_recv, s_send, s_recv, a_send, a_recv, f_send, f_recv):
    t = lax.axis_index("tp")
    j = lax.axis_index("kvp")
    core = lax.rem(j, 2)
    xpos = j // 2
    quarter = t * 2 + xpos
    mate = {"tp": t, "kvp": j + 1 - 2 * core}
    chips = []
    for e in (1, 2, 3):
        tt = t if e == 1 else 1 - t
        xx = xpos if e == 2 else 1 - xpos
        chips.append(({"tp": tt, "kvp": xx * 2 + core}, tt * 2 + xx))
    ring = [{"tp": t, "kvp": lax.rem(j + d, 4)} for d in (1, 2, 3)]

    wo_copy = pltpu.make_async_copy(wo_hbm, wo, w_sem)
    wo_copy.start()
    enter(tuple(ring) + (chips[1][0], chips[2][0]))

    def combine_copy(d):
        return remote(part_ref.at[lax.rem(j + d, 4)], rx.at[d - 1], c_send.at[d - 1], c_recv.at[d - 1], ring[d - 1])

    for d in (2, 1, 3):
        combine_copy(d).start()

    full = FFL // GCH
    rest = FFL - full * GCH
    spans = [(i * GCH, GCH) for i in range(full)] + [(full * GCH, rest)]

    def gate_copy(i, which):
        first, n = spans[i]
        src, dst = ((wg_hbm, wg), (wu_hbm, wu))[which]
        return pltpu.make_async_copy(src.at[pl.ds(first, n)], dst.at[pl.ds(first, n)], gu_sem.at[which, i])

    def down_copy(i):
        rows = pl.ds(i * (FFL // 4), FFL // 4)
        return pltpu.make_async_copy(wd_hbm.at[rows], wd.at[rows], wd_sem.at[i])

    wo_copy.wait()
    for i in range(len(spans)):
        gate_copy(i, 0).start()
        gate_copy(i, 1).start()
    for i in range(4):
        down_copy(i).start()

    for d in (1, 2, 3):
        combine_copy(d).wait_recv()
    stats = [part_ref[j, GRP]] + [rx[i, GRP] for i in range(3)]
    for r in range(GRP):
        ms = [s[:, r:r + 1] for s in stats]
        top = jnp.maximum(jnp.maximum(ms[0], ms[1]), jnp.maximum(ms[2], ms[3]))
        scales = [jnp.exp(m - top) for m in ms]
        denom = sum(sc * s[:, 8 + r:9 + r] for sc, s in zip(scales, stats))
        total = part_ref[j, r] * scales[0]
        for i in range(3):
            total = total + rx[i, r] * scales[i + 1]
        attn[:, r * HD:(r + 1) * HD] = (total / denom).astype(BF16)

    def all_sum(which, product, base, pair, rs, ag):
        def pair_copy(k):
            return remote(pbuf.at[k, pl.ds((1 - core) * 4, 4)], pair.at[k], d_send.at[which, k], d_recv.at[which, k], mate)

        def scatter_copy(k, e):
            dev, q = chips[e]
            return remote(sbuf.at[k, q], rs.at[k, e], s_send.at[which, k, e], s_recv.at[which, k, e], dev)

        own = core * 4 + quarter

        def gather_copy(k, e):
            dev = mate if e == 3 else chips[e][0]
            return remote(ag.at[k * 8 + own], ag.at[k * 8 + own], a_send.at[which, k, e], a_recv.at[which, k, e], dev)

        def forward_copy(k, e):
            slot = k * 8 + core * 4 + chips[e][1]
            return remote(ag.at[slot], ag.at[slot], f_send.at[which, k, e], f_recv.at[which, k, e], mate)

        for k in range(NCH):
            res = product(k)
            for i in range(8):
                pbuf[k, i] = res[:, i * HD:(i + 1) * HD]
            pair_copy(k).start()
        for k in range(NCH):
            pair_copy(k).wait_recv()
            for i in range(4):
                sbuf[k, i] = pbuf[k, core * 4 + i] + pair[k, i]
            for e in (2, 0, 1):
                scatter_copy(k, e).start()
        for k in range(NCH):
            for e in range(3):
                scatter_copy(k, e).wait_recv()
            total = sbuf[k, quarter] + rs[k, 0] + rs[k, 1] + rs[k, 2]
            ag[k * 8 + own] = (base(k * 8 + own) + total).astype(BF16).astype(F32)
            for e in (2, 0, 1, 3):
                gather_copy(k, e).start()
        for k in range(NCH):
            for e in range(3):
                gather_copy(k, e).wait_recv()
                forward_copy(k, e).start()
        for k in range(NCH):
            gather_copy(k, 3).wait_recv()
            for e in range(3):
                forward_copy(k, e).wait_recv()
        for k in range(NCH):
            pair_copy(k).wait_send()
            for e in range(3):
                scatter_copy(k, e).wait_send()
                forward_copy(k, e).wait_send()
            for e in range(4):
                gather_copy(k, e).wait_send()

    def o_product(k):
        return jnp.dot(attn[...], wo[:, k * CW:(k + 1) * CW], preferred_element_type=F32)

    def x_base(i):
        return x_ref[:, pl.ds(pl.multiple_of(i * HD, HD), HD)].astype(F32)

    all_sum(0, o_product, x_base, pair_a, rs_a, ag_a)

    squares = jnp.zeros((B, HD), F32)
    for i in range(D // HD):
        squares = squares + ag_a[i] * ag_a[i]
    inv = lax.rsqrt(jnp.sum(squares, axis=-1, keepdims=True) / D + EPS)
    for i in range(D // HD):
        cols = slice(i * HD, (i + 1) * HD)
        n_ref[:, cols] = (ag_a[i] * inv * g_ref[:, cols].astype(F32)).astype(BF16)

    def gate_step(first, n):
        dims = (((1,), (1,)), ((), ()))
        gate = lax.dot_general(n_ref[...], wg[pl.ds(first, n), :], dims, preferred_element_type=F32)
        up = lax.dot_general(n_ref[...], wu[pl.ds(first, n), :], dims, preferred_element_type=F32)
        return (jax.nn.silu(gate) * up).astype(BF16)

    for i, (first, n) in enumerate(spans):
        gate_copy(i, 0).wait()
        gate_copy(i, 1).wait()
        y_ref[:, first:first + n] = gate_step(first, n)
    for i in range(4):
        down_copy(i).wait()

    def down_product(k):
        return jnp.dot(y_ref[...], wd[:, k * CW:(k + 1) * CW], preferred_element_type=F32)

    all_sum(1, down_product, lambda i: ag_a[i], pair_b, rs_b, ag_b)
    for i in range(D // HD):
        out_ref[:, i * HD:(i + 1) * HD] = ag_b[i].astype(BF16)
    for d in (1, 2, 3):
        combine_copy(d).wait_send()


def vmem():
    return pl.BlockSpec(memory_space=pltpu.VMEM)


def hbm():
    return pl.BlockSpec(memory_space=pl.ANY)


def dma(*shape):
    return pltpu.SemaphoreType.DMA(shape)


def layer_step(x_in, ctx_len, g_attn, g_mlp, w_qkv, w_o, w_gate, w_up, w_down, k_cache, v_cache):
    inv_freq = ROPE_THETA ** (-2.0 * jnp.arange(HD // 2, dtype=F32) / HD)
    angles = ctx_len.astype(F32)[:, None] * inv_freq[None, :]
    cos_t, sin_t = jnp.cos(angles), jnp.sin(angles)
    cos_t = jnp.concatenate([cos_t, cos_t], axis=1)
    sin_t = jnp.concatenate([-sin_t, sin_t], axis=1)
    nch = len(CHUNKS)
    q2, kn, vn = pl.pallas_call(
        qkv_kernel,
        out_shape=(jax.ShapeDtypeStruct((B * ROWS, HD), F32), jax.ShapeDtypeStruct((B * 8, HD), F32), jax.ShapeDtypeStruct((B * 8, HD), F32)),
        in_specs=[vmem(), vmem(), vmem(), vmem(), hbm()],
        out_specs=(vmem(), vmem(), vmem()),
        scratch_shapes=[
            pltpu.VMEM((D, QCOLS), BF16), pltpu.VMEM((B, D), BF16), pltpu.VMEM((KVL, GRP + 2, B, HD), F32),
            dma(nch), dma(nch), dma(nch), dma(nch), dma(nch), dma(nch), dma(nch),
        ],
        compiler_params=pltpu.CompilerParams(collective_id=0, has_side_effects=True),
        name="qkv",
    )(x_in, g_attn.reshape(1, D), cos_t, sin_t, w_qkv)

    kc = k_cache.reshape(B, T * KVL, HD)
    vc = v_cache.reshape(B, T * KVL, HD)
    part, k_out, v_out = pl.pallas_call(
        attn_kernel,
        out_shape=(jax.ShapeDtypeStruct((KVL, GRP + 1, B, HD), F32), jax.ShapeDtypeStruct(kc.shape, BF16), jax.ShapeDtypeStruct(vc.shape, BF16)),
        in_specs=[pl.BlockSpec(memory_space=pltpu.SMEM), vmem(), vmem(), vmem(), hbm(), hbm()],
        out_specs=(vmem(), hbm(), hbm()),
        scratch_shapes=[
            pltpu.VMEM(kc.shape, BF16), pltpu.VMEM(vc.shape, BF16), pltpu.VMEM((2 * ROWS, KVL * T), F32),
            pltpu.VMEM((B * ROWS, HD), F32), pltpu.VMEM((B * ROWS, HD), F32), pltpu.VMEM((B * ROWS, HD), F32),
            dma(2, PAIRS), dma(2, PAIRS),
        ],
        name="attn",
    )(ctx_len, q2, kn, vn, kc, vc)

    x_out = pl.pallas_call(
        tail_kernel,
        out_shape=jax.ShapeDtypeStruct((B, D), BF16),
        in_specs=[vmem(), vmem(), vmem(), hbm(), hbm(), hbm(), hbm()],
        out_specs=vmem(),
        scratch_shapes=[
            pltpu.VMEM(w_o.shape, BF16), pltpu.VMEM((FFL, D), BF16), pltpu.VMEM((FFL, D), BF16), pltpu.VMEM((FFL, D), BF16),
            pltpu.VMEM((3, GRP + 1, B, HD), F32), pltpu.VMEM((B, GRP * HD), BF16), pltpu.VMEM((B, D), BF16), pltpu.VMEM((B, FFL), BF16),
            pltpu.VMEM((NCH, 8, B, HD), F32), pltpu.VMEM((NCH, 4, B, HD), F32),
            pltpu.VMEM((NCH, 4, B, HD), F32), pltpu.VMEM((NCH, 4, B, HD), F32),
            pltpu.VMEM((NCH, 3, B, HD), F32), pltpu.VMEM((NCH, 3, B, HD), F32),
            pltpu.VMEM((D // HD, B, HD), F32), pltpu.VMEM((D // HD, B, HD), F32),
            pltpu.SemaphoreType.DMA, dma(2, 7), dma(4), dma(3), dma(3),
            dma(2, NCH), dma(2, NCH), dma(2, NCH, 3), dma(2, NCH, 3), dma(2, NCH, 4), dma(2, NCH, 4), dma(2, NCH, 3), dma(2, NCH, 3),
        ],
        compiler_params=pltpu.CompilerParams(collective_id=1, has_side_effects=True, vmem_limit_bytes=VMEM_MAX),
        name="tail",
    )(part, x_in, g_mlp.reshape(1, D), w_o, w_gate.T, w_up.T, w_down)
    return x_out, k_out.reshape(k_cache.shape), v_out.reshape(v_cache.shape)


def solution(mesh):
    x_spec = P("dp", None)
    cache_spec = P("dp", "kvp", "tp", None)
    model_axes = ("tp", "kvp")
    in_specs = (x_spec, P("dp"), P(None), P(None), P(None, "tp"), P(model_axes, None), P(None, model_axes), P(None, model_axes), P(model_axes, None), cache_spec, cache_spec)
    return jax.shard_map(layer_step, mesh=mesh, in_specs=in_specs, out_specs=(x_spec, cache_spec, cache_spec), check_vma=False)
```

```python
import jax
import jax.numpy as jnp
import numpy as np
from jax import lax
from jax.experimental import pallas as pl
from jax.experimental.pallas import tpu as pltpu
from jax.sharding import PartitionSpec as P

ROPE_THETA = 500000.0
EPS = 1e-5
NEG_FILL = -1e30
MESH = pl.DeviceIdType.MESH
F32 = jnp.float32
BF16 = jnp.bfloat16

D = 5120
HD = 128
B = 32
T = 256
KVL = 4
GRP = 5
ROWS = 24
QCOLS = (GRP + 2) * HD
FFL = 1728
MIB = 1024 * 1024
TAIL_VMEM = 56 * MIB


def remote(src, dst, send, recv, dev):
    return pltpu.make_async_remote_copy(src_ref=src, dst_ref=dst, send_sem=send, recv_sem=recv, device_id=dev, device_id_type=MESH)


def enter(peers):
    barrier = pltpu.get_barrier_semaphore()
    for peer in peers:
        pl.semaphore_signal(barrier, inc=1, device_id=peer, device_id_type=MESH)
    pl.semaphore_wait(barrier, len(peers))


CHUNKS = ((0, 2), (2, 2), (4, 2), (6, 1))


def qkv_kernel(ctx_ref, freq_ref, x_hbm, g_hbm, w_ref, k_hbm, v_hbm, q_ref, kn_ref, vn_ref, kc_ref, vc_ref,
               x_ref, g_ref, wbuf, u_ref, ex, x_sem, w_sem, c_sem, m_send, m_recv, x_send, x_recv, r_send, r_recv):
    j = lax.axis_index("kvp")
    mate = {"kvp": j + 1 - 2 * lax.rem(j, 2)}
    side = {"kvp": lax.rem(j + 2, 4)}
    x_copy = pltpu.make_async_copy(x_hbm, x_ref, x_sem.at[0])
    g_copy = pltpu.make_async_copy(g_hbm, g_ref, x_sem.at[1])
    x_copy.start()
    g_copy.start()

    def cache_copy(i):
        src, dst = ((k_hbm, kc_ref), (v_hbm, vc_ref))[i // 4]
        some = pl.ds((i % 4) * 8, 8)
        return pltpu.make_async_copy(src.at[some], dst.at[some], c_sem.at[i])

    def load(i):
        first, n = CHUNKS[i]
        cols = pl.ds(pl.multiple_of(j * QCOLS + first * HD, HD), n * HD)
        return pltpu.make_async_copy(w_ref.at[:, cols], wbuf.at[:, pl.ds(first * HD, n * HD)], w_sem.at[i])

    load(0).start()
    load(1).start()
    enter((mate, side))
    row = lax.broadcasted_iota(jnp.int32, (B, HD), 0)
    lane = lax.broadcasted_iota(jnp.int32, (B, HD), 1)
    ctx = jnp.zeros((B, HD), F32)
    for b in range(B):
        ctx = jnp.where(row == b, ctx_ref[b].astype(F32), ctx)
    angles = ctx * freq_ref[...]
    cos_t = jnp.cos(angles)
    sin_t = jnp.sin(angles)
    sin_t = jnp.where(lane < HD // 2, -sin_t, sin_t)
    x_copy.wait()
    g_copy.wait()
    squares = jnp.zeros((B, HD), F32)
    for i in range(D // HD):
        xf = x_ref[:, i * HD:(i + 1) * HD].astype(F32)
        squares = squares + xf * xf
    inv = lax.rsqrt(jnp.sum(squares, axis=-1, keepdims=True) / D + EPS)
    for i in range(D // HD):
        xf = x_ref[:, i * HD:(i + 1) * HD].astype(F32)
        u_ref[:, i * HD:(i + 1) * HD] = (xf * inv * g_ref[i:i + 1, :].astype(F32)).astype(BF16)
    q_ref[...] = jnp.zeros_like(q_ref)

    def piece(slot, i):
        first, n = CHUNKS[i]
        return ex.at[slot, pl.ds(first, n)]

    def to_mate(i):
        return remote(piece(j, i), piece(j, i), m_send.at[i], m_recv.at[i], mate)

    def to_side(i):
        return remote(piece(j, i), piece(j, i), x_send.at[i], x_recv.at[i], side)

    def relay(i):
        slot = lax.rem(j + 2, 4)
        return remote(piece(slot, i), piece(slot, i), r_send.at[i], r_recv.at[i], mate)

    for i, (first, n) in enumerate(CHUNKS):
        load(i).wait()
        if i + 2 < len(CHUNKS):
            load(i + 2).start()
        else:
            for c in range((i - 2) * 4, (i - 1) * 4):
                cache_copy(c).start()
        res = jnp.dot(u_ref[...], wbuf[:, first * HD:(first + n) * HD], preferred_element_type=F32)
        for h in range(n):
            tile = res[:, h * HD:(h + 1) * HD]
            if first + h < GRP + 1:
                tile = tile * cos_t + pltpu.roll(tile, HD // 2, 1) * sin_t
            ex[j, first + h] = tile
        to_side(i).start()
        to_mate(i).start()
    for i in range(len(CHUNKS)):
        to_side(i).wait_recv()
        relay(i).start()
    for i in range(len(CHUNKS)):
        to_mate(i).wait_recv()
        relay(i).wait_recv()
    for g in range(KVL):
        for r in range(GRP):
            q_ref[pl.ds(g * GRP + r, B, stride=ROWS), :] = ex[g, r]
        kn = ex[g, GRP]
        vn = ex[g, GRP + 1]
        for half in range(2):
            kn_ref[pl.ds(half * KVL + g, B, stride=8), :] = kn
            vn_ref[pl.ds(half * KVL + g, B, stride=8), :] = vn
    for i in range(len(CHUNKS)):
        to_side(i).wait_send()
        to_mate(i).wait_send()
        relay(i).wait_send()
    for i in range(8):
        cache_copy(i).wait()


PAIRS = B // 2


def attn_kernel(ctx_ref, q_ref, kn_ref, vn_ref, k_ref, v_ref, part_ref, kbuf, vbuf, ko_ref, vo_ref, bias, acc2, m2, l2, out_sem):
    base = lax.axis_index("kvp") * T

    def flush(i, which):
        src, dst = ((kbuf, ko_ref), (vbuf, vo_ref))[which]
        some = pl.ds(4 * i, 4)
        return pltpu.make_async_copy(src.at[some], dst.at[some], out_sem.at[which, i])

    row = lax.broadcasted_iota(jnp.int32, (2 * ROWS, KVL * T), 0)
    row = jnp.where(row >= ROWS, row - ROWS, row)
    col = lax.broadcasted_iota(jnp.int32, (2 * ROWS, KVL * T), 1)
    head = (row >= GRP).astype(jnp.int32) + (row >= 2 * GRP).astype(jnp.int32) + (row >= 3 * GRP).astype(jnp.int32)
    bias[...] = jnp.where(head == (col & (KVL - 1)), 0.0, NEG_FILL)
    first_half = lax.broadcasted_iota(jnp.int32, (2 * ROWS, 1), 0) < ROWS
    wrow = lax.broadcasted_iota(jnp.int32, (16, HD), 0)

    def patch(b):
        pos = ctx_ref[b] - base

        @pl.when((pos >= 0) & (pos < T))
        def _():
            win = pl.ds(pl.multiple_of((pos // 4) * 16, 16), 16)
            hit = (wrow // KVL) == (pos & 3)
            for new_ref, buf in ((kn_ref, kbuf), (vn_ref, vbuf)):
                new8 = new_ref[pl.ds(b * 8, 8), :]
                new16 = jnp.concatenate([new8, new8], axis=0)
                buf[b, win, :] = jnp.where(hit, new16, buf[b, win, :].astype(F32)).astype(BF16)

    def attend(p):
        b = 2 * p
        q = q_ref[pl.ds(p * 2 * ROWS, 2 * ROWS), :]
        lhs = jnp.concatenate([jnp.where(first_half, q, 0.0), jnp.where(first_half, 0.0, q)], axis=1).astype(BF16)
        keys = jnp.concatenate([kbuf[b], kbuf[b + 1]], axis=1)
        s = lax.dot_general(lhs, keys, (((1,), (1,)), ((), ())), preferred_element_type=F32)
        lim = jnp.where(first_half, (ctx_ref[b] - base + 1) * KVL, (ctx_ref[b + 1] - base + 1) * KVL)
        cols = lax.broadcasted_iota(jnp.int32, (2 * ROWS, KVL * T), 1)
        s = jnp.where(cols < lim, s * HD ** -0.5 + bias[...], NEG_FILL)
        m = jnp.max(s, axis=1, keepdims=True)
        w = jnp.exp(s - m)
        values = jnp.concatenate([vbuf[b], vbuf[b + 1]], axis=1)
        o = jnp.dot(w.astype(BF16), values, preferred_element_type=F32)
        rows = pl.ds(p * 2 * ROWS, 2 * ROWS)
        acc2[rows, :] = jnp.where(first_half, o[:, :HD], o[:, HD:])
        m2[rows, :] = jnp.broadcast_to(m, (2 * ROWS, HD))
        l2[rows, :] = jnp.broadcast_to(jnp.sum(w, axis=1, keepdims=True), (2 * ROWS, HD))

    @pl.loop(0, B // 4)
    def _(it):
        for k in range(4):
            patch(it * 4 + k)
        flush(it, 0).start()
        flush(it, 1).start()

    @pl.loop(0, PAIRS // 2)
    def _(it):
        for k in range(2):
            attend(it * 2 + k)

    lane = lax.broadcasted_iota(jnp.int32, (B, HD), 1)
    for g in range(KVL):
        stats = jnp.zeros((B, HD), F32)
        for r in range(GRP):
            rows = pl.ds(g * GRP + r, B, stride=ROWS)
            part_ref[g, r] = acc2[rows, :]
            stats = jnp.where(lane == r, m2[rows, :], stats)
            stats = jnp.where(lane == 8 + r, l2[rows, :], stats)
        part_ref[g, GRP] = stats

    @pl.loop(0, B // 4)
    def _(i):
        flush(i, 0).wait()
        flush(i, 1).wait()


NCH = 5
CW = D // NCH
GCH = 256


def tail_kernel(part_ref, x_hbm, g_hbm, wo_hbm, wg_hbm, wu_hbm, wd_hbm, out_ref,
                x_ref, g_ref, wo, wg, wu, rx, attn, n_ref, y_ref, pbuf, sbuf, pair_a, pair_b, rs_a, rs_b, ag_a, ag_b,
                x_sem, w_sem, gu_sem, wd_sem, c_send, c_recv, d_send, d_recv, s_send, s_recv, a_send, a_recv, f_send, f_recv):
    t = lax.axis_index("tp")
    j = lax.axis_index("kvp")
    core = lax.rem(j, 2)
    xpos = j // 2
    quarter = t * 2 + xpos
    mate = {"tp": t, "kvp": j + 1 - 2 * core}
    chips = []
    for e in (1, 2, 3):
        tt = t if e == 1 else 1 - t
        xx = xpos if e == 2 else 1 - xpos
        chips.append(({"tp": tt, "kvp": xx * 2 + core}, tt * 2 + xx))
    ring = [{"tp": t, "kvp": lax.rem(j + d, 4)} for d in (1, 2, 3)]

    wo_copy = pltpu.make_async_copy(wo_hbm, wo, w_sem)
    wo_copy.start()
    x_copy = pltpu.make_async_copy(x_hbm, x_ref, x_sem.at[0])
    g_copy = pltpu.make_async_copy(g_hbm, g_ref, x_sem.at[1])
    x_copy.start()
    g_copy.start()
    enter(tuple(ring) + (chips[1][0], chips[2][0]))

    def combine_copy(d):
        return remote(part_ref.at[lax.rem(j + d, 4)], rx.at[d - 1], c_send.at[d - 1], c_recv.at[d - 1], ring[d - 1])

    for d in (2, 1, 3):
        combine_copy(d).start()

    full = FFL // GCH
    rest = FFL - full * GCH
    spans = [(i * GCH, GCH) for i in range(full)] + [(full * GCH, rest)]

    def gate_copy(i, which):
        first, n = spans[i]
        src, dst = ((wg_hbm, wg), (wu_hbm, wu))[which]
        return pltpu.make_async_copy(src.at[pl.ds(first, n)], dst.at[pl.ds(first, n)], gu_sem.at[which, i])

    def down_copy(i):
        rows = pl.ds(*spans[i])
        return pltpu.make_async_copy(wd_hbm.at[rows], wg.at[rows], wd_sem.at[i])

    wo_copy.wait()
    x_copy.wait()
    g_copy.wait()
    for i in range(len(spans)):
        gate_copy(i, 0).start()
        gate_copy(i, 1).start()

    for d in (1, 2, 3):
        combine_copy(d).wait_recv()
    stats = [part_ref[j, GRP]] + [rx[i, GRP] for i in range(3)]
    for r in range(GRP):
        ms = [s[:, r:r + 1] for s in stats]
        top = jnp.maximum(jnp.maximum(ms[0], ms[1]), jnp.maximum(ms[2], ms[3]))
        scales = [jnp.exp(m - top) for m in ms]
        denom = sum(sc * s[:, 8 + r:9 + r] for sc, s in zip(scales, stats))
        total = part_ref[j, r] * scales[0]
        for i in range(3):
            total = total + rx[i, r] * scales[i + 1]
        attn[:, r * HD:(r + 1) * HD] = (total / denom).astype(BF16)

    def all_sum(which, product, base, pair, rs, ag):
        def pair_copy(k):
            return remote(pbuf.at[k, pl.ds((1 - core) * 4, 4)], pair.at[k], d_send.at[which, k], d_recv.at[which, k], mate)

        def scatter_copy(k, e):
            dev, q = chips[e]
            return remote(sbuf.at[k, q], rs.at[k, e], s_send.at[which, k, e], s_recv.at[which, k, e], dev)

        own = core * 4 + quarter

        def gather_copy(k, e):
            dev = mate if e == 3 else chips[e][0]
            return remote(ag.at[k * 8 + own], ag.at[k * 8 + own], a_send.at[which, k, e], a_recv.at[which, k, e], dev)

        def forward_copy(k, e):
            slot = k * 8 + core * 4 + chips[e][1]
            return remote(ag.at[slot], ag.at[slot], f_send.at[which, k, e], f_recv.at[which, k, e], mate)

        for k in range(NCH):
            res = product(k)
            for i in range(8):
                pbuf[k, i] = res[:, i * HD:(i + 1) * HD]
            pair_copy(k).start()
        for k in range(NCH):
            pair_copy(k).wait_recv()
            for i in range(4):
                sbuf[k, i] = pbuf[k, core * 4 + i] + pair[k, i]
            for e in (2, 0, 1):
                scatter_copy(k, e).start()
        for k in range(NCH):
            for e in range(3):
                scatter_copy(k, e).wait_recv()
            total = sbuf[k, quarter] + rs[k, 0] + rs[k, 1] + rs[k, 2]
            ag[k * 8 + own] = (base(k * 8 + own) + total).astype(BF16).astype(F32)
            for e in (2, 0, 1, 3):
                gather_copy(k, e).start()
        for k in range(NCH):
            for e in range(3):
                gather_copy(k, e).wait_recv()
                forward_copy(k, e).start()
        for k in range(NCH):
            gather_copy(k, 3).wait_recv()
            for e in range(3):
                forward_copy(k, e).wait_recv()
        for k in range(NCH):
            pair_copy(k).wait_send()
            for e in range(3):
                scatter_copy(k, e).wait_send()
                forward_copy(k, e).wait_send()
            for e in range(4):
                gather_copy(k, e).wait_send()

    def o_product(k):
        return jnp.dot(attn[...], wo[:, k * CW:(k + 1) * CW], preferred_element_type=F32)

    def x_base(i):
        return x_ref[:, pl.ds(pl.multiple_of(i * HD, HD), HD)].astype(F32)

    all_sum(0, o_product, x_base, pair_a, rs_a, ag_a)

    squares = jnp.zeros((B, HD), F32)
    for i in range(D // HD):
        squares = squares + ag_a[i] * ag_a[i]
    inv = lax.rsqrt(jnp.sum(squares, axis=-1, keepdims=True) / D + EPS)
    for i in range(D // HD):
        n_ref[:, i * HD:(i + 1) * HD] = (ag_a[i] * inv * g_ref[i:i + 1, :].astype(F32)).astype(BF16)

    def gate_step(first, n):
        dims = (((1,), (1,)), ((), ()))
        gate = lax.dot_general(n_ref[...], wg[pl.ds(first, n), :], dims, preferred_element_type=F32)
        up = lax.dot_general(n_ref[...], wu[pl.ds(first, n), :], dims, preferred_element_type=F32)
        return (jax.nn.silu(gate) * up).astype(BF16)

    for i, (first, n) in enumerate(spans):
        gate_copy(i, 0).wait()
        gate_copy(i, 1).wait()
        y_ref[:, first:first + n] = gate_step(first, n)
        down_copy(i).start()
    for i in range(len(spans)):
        down_copy(i).wait()

    def down_product(k):
        return jnp.dot(y_ref[...], wg[:, k * CW:(k + 1) * CW], preferred_element_type=F32)

    all_sum(1, down_product, lambda i: ag_a[i], pair_b, rs_b, ag_b)
    for i in range(D // HD):
        out_ref[:, i * HD:(i + 1) * HD] = ag_b[i].astype(BF16)
    for d in (1, 2, 3):
        combine_copy(d).wait_send()


def vmem():
    return pl.BlockSpec(memory_space=pltpu.VMEM)


def hbm():
    return pl.BlockSpec(memory_space=pl.ANY)


def in_hbm(a):
    return pltpu.with_memory_space_constraint(a, pltpu.HBM)


def in_vmem(a):
    return pltpu.with_memory_space_constraint(a, pltpu.VMEM)


def smem():
    return pl.BlockSpec(memory_space=pltpu.SMEM)


def dma(*shape):
    return pltpu.SemaphoreType.DMA(shape)


def layer_step(x_in, ctx_len, g_attn, g_mlp, w_qkv, w_o, w_gate, w_up, w_down, k_cache, v_cache):
    freq = ROPE_THETA ** (-2.0 * np.arange(HD // 2, dtype=np.float64) / HD)
    freq = np.concatenate([freq, freq]).astype(np.float32).reshape(1, HD)
    kc = k_cache.reshape(B, T * KVL, HD)
    vc = v_cache.reshape(B, T * KVL, HD)
    nch = len(CHUNKS)
    q2, kn, vn, kc, vc = pl.pallas_call(
        qkv_kernel,
        out_shape=(pltpu.VMEM((B * ROWS, HD), F32), pltpu.VMEM((B * 8, HD), F32), pltpu.VMEM((B * 8, HD), F32),
                   pltpu.VMEM(kc.shape, BF16), pltpu.VMEM(vc.shape, BF16)),
        in_specs=[smem(), vmem(), hbm(), hbm(), hbm(), hbm(), hbm()],
        out_specs=(vmem(),) * 5,
        scratch_shapes=[
            pltpu.VMEM((B, D), BF16), pltpu.VMEM((D // HD, HD), BF16),
            pltpu.VMEM((D, QCOLS), BF16), pltpu.VMEM((B, D), BF16), pltpu.VMEM((KVL, GRP + 2, B, HD), F32),
            dma(2), dma(nch), dma(8), dma(nch), dma(nch), dma(nch), dma(nch), dma(nch), dma(nch),
        ],
        compiler_params=pltpu.CompilerParams(collective_id=0, has_side_effects=True, vmem_limit_bytes=MIB * 16),
        name="qkv",
    )(in_hbm(ctx_len), in_hbm(freq), in_hbm(x_in), in_hbm(g_attn.reshape(D // HD, HD)), in_hbm(w_qkv), in_hbm(kc), in_hbm(vc))

    part, kc, vc, k_out, v_out = pl.pallas_call(
        attn_kernel,
        out_shape=(pltpu.VMEM((KVL, GRP + 1, B, HD), F32), pltpu.VMEM(kc.shape, BF16), pltpu.VMEM(vc.shape, BF16),
                   jax.ShapeDtypeStruct(kc.shape, BF16), jax.ShapeDtypeStruct(vc.shape, BF16)),
        in_specs=[smem(), vmem(), vmem(), vmem(), vmem(), vmem()],
        out_specs=(vmem(), vmem(), vmem(), hbm(), hbm()),
        scratch_shapes=[
            pltpu.VMEM((2 * ROWS, KVL * T), F32),
            pltpu.VMEM((B * ROWS, HD), F32), pltpu.VMEM((B * ROWS, HD), F32), pltpu.VMEM((B * ROWS, HD), F32),
            dma(2, B // 4),
        ],
        input_output_aliases={4: 1, 5: 2},
        compiler_params=pltpu.CompilerParams(vmem_limit_bytes=MIB * 4),
        name="attn",
    )(in_hbm(ctx_len), q2, kn, vn, kc, vc)

    x_out = pl.pallas_call(
        tail_kernel,
        out_shape=pltpu.VMEM((B, D), BF16),
        in_specs=[vmem(), hbm(), hbm(), hbm(), hbm(), hbm(), hbm()],
        out_specs=vmem(),
        scratch_shapes=[
            pltpu.VMEM((B, D), BF16), pltpu.VMEM((D // HD, HD), BF16), pltpu.VMEM(w_o.shape, BF16), pltpu.VMEM((FFL, D), BF16), pltpu.VMEM((FFL, D), BF16),
            pltpu.VMEM((3, GRP + 1, B, HD), F32), pltpu.VMEM((B, GRP * HD), BF16), pltpu.VMEM((B, D), BF16), pltpu.VMEM((B, FFL), BF16),
            pltpu.VMEM((NCH, 8, B, HD), F32), pltpu.VMEM((NCH, 4, B, HD), F32),
            pltpu.VMEM((NCH, 4, B, HD), F32), pltpu.VMEM((NCH, 4, B, HD), F32),
            pltpu.VMEM((NCH, 3, B, HD), F32), pltpu.VMEM((NCH, 3, B, HD), F32),
            pltpu.VMEM((D // HD, B, HD), F32), pltpu.VMEM((D // HD, B, HD), F32),
            dma(2), pltpu.SemaphoreType.DMA, dma(2, 7), dma(7), dma(3), dma(3),
            dma(2, NCH), dma(2, NCH), dma(2, NCH, 3), dma(2, NCH, 3), dma(2, NCH, 4), dma(2, NCH, 4), dma(2, NCH, 3), dma(2, NCH, 3),
        ],
        compiler_params=pltpu.CompilerParams(collective_id=1, has_side_effects=True, vmem_limit_bytes=TAIL_VMEM),
        cost_estimate=pl.CostEstimate(flops=10 ** 10, bytes_accessed=10 ** 8, transcendentals=0),
        name="tail",
    )(in_vmem(part), in_hbm(x_in), in_hbm(g_mlp.reshape(D // HD, HD)), in_hbm(w_o), in_hbm(w_gate.T), in_hbm(w_up.T), in_hbm(w_down))
    return x_out, k_out.reshape(k_cache.shape), v_out.reshape(v_cache.shape)


def solution(mesh):
    x_spec = P("dp", None)
    cache_spec = P("dp", "kvp", "tp", None)
    model_axes = ("tp", "kvp")
    in_specs = (x_spec, P("dp"), P(None), P(None), P(None, "tp"), P(model_axes, None), P(None, model_axes), P(None, model_axes), P(model_axes, None), cache_spec, cache_spec)
    return jax.shard_map(layer_step, mesh=mesh, in_specs=in_specs, out_specs=(x_spec, cache_spec, cache_spec), check_vma=False)
```

```python
import jax
import jax.numpy as jnp
import numpy as np
from jax import lax
from jax.experimental import pallas as pl
from jax.experimental.pallas import tpu as pltpu
from jax.sharding import PartitionSpec as P

ROPE_THETA = 500000.0
EPS = 1e-5
NEG_FILL = -1e30
MESH = pl.DeviceIdType.MESH
F32 = jnp.float32
BF16 = jnp.bfloat16

D = 5120
HD = 128
B = 32
T = 256
KVL = 4
GRP = 5
ROWS = 24
QCOLS = (GRP + 2) * HD
FFL = 1728
MIB = 1024 * 1024
TAIL_VMEM = 56 * MIB


def remote(src, dst, send, recv, dev):
    return pltpu.make_async_remote_copy(src_ref=src, dst_ref=dst, send_sem=send, recv_sem=recv, device_id=dev, device_id_type=MESH)


def enter(peers):
    barrier = pltpu.get_barrier_semaphore()
    for peer in peers:
        pl.semaphore_signal(barrier, inc=1, device_id=peer, device_id_type=MESH)
    pl.semaphore_wait(barrier, len(peers))


CHUNKS = ((0, 2), (2, 2), (4, 2), (6, 1))


def qkv_kernel(ctx_ref, freq_ref, x_hbm, g_hbm, w_ref, k_hbm, v_hbm, q_ref, kn_ref, vn_ref, kc_ref, vc_ref,
               x_ref, g_ref, wbuf, u_ref, ex, x_sem, w_sem, c_sem, m_send, m_recv, x_send, x_recv, r_send, r_recv):
    j = lax.axis_index("kvp")
    mate = {"kvp": j + 1 - 2 * lax.rem(j, 2)}
    side = {"kvp": lax.rem(j + 2, 4)}
    x_copy = pltpu.make_async_copy(x_hbm, x_ref, x_sem.at[0])
    g_copy = pltpu.make_async_copy(g_hbm, g_ref, x_sem.at[1])
    x_copy.start()
    g_copy.start()

    def cache_copy(i):
        src, dst = ((k_hbm, kc_ref), (v_hbm, vc_ref))[i // 4]
        some = pl.ds((i % 4) * 8, 8)
        return pltpu.make_async_copy(src.at[some], dst.at[some], c_sem.at[i])

    def load(i):
        first, n = CHUNKS[i]
        cols = pl.ds(pl.multiple_of(j * QCOLS + first * HD, HD), n * HD)
        return pltpu.make_async_copy(w_ref.at[:, cols], wbuf.at[:, pl.ds(first * HD, n * HD)], w_sem.at[i])

    load(0).start()
    load(1).start()
    enter((mate, side))
    row = lax.broadcasted_iota(jnp.int32, (B, HD), 0)
    lane = lax.broadcasted_iota(jnp.int32, (B, HD), 1)
    ctx = jnp.zeros((B, HD), F32)
    for b in range(B):
        ctx = jnp.where(row == b, ctx_ref[b].astype(F32), ctx)
    angles = ctx * freq_ref[...]
    cos_t = jnp.cos(angles)
    sin_t = jnp.sin(angles)
    sin_t = jnp.where(lane < HD // 2, -sin_t, sin_t)
    x_copy.wait()
    g_copy.wait()
    squares = jnp.zeros((B, HD), F32)
    for i in range(D // HD):
        xf = x_ref[:, i * HD:(i + 1) * HD].astype(F32)
        squares = squares + xf * xf
    inv = lax.rsqrt(jnp.sum(squares, axis=-1, keepdims=True) / D + EPS)
    for i in range(D // HD):
        xf = x_ref[:, i * HD:(i + 1) * HD].astype(F32)
        u_ref[:, i * HD:(i + 1) * HD] = (xf * inv * g_ref[i:i + 1, :].astype(F32)).astype(BF16)
    q_ref[...] = jnp.zeros_like(q_ref)

    def piece(slot, i):
        first, n = CHUNKS[i]
        return ex.at[slot, pl.ds(first, n)]

    def to_mate(i):
        return remote(piece(j, i), piece(j, i), m_send.at[i], m_recv.at[i], mate)

    def to_side(i):
        return remote(piece(j, i), piece(j, i), x_send.at[i], x_recv.at[i], side)

    def relay(i):
        slot = lax.rem(j + 2, 4)
        return remote(piece(slot, i), piece(slot, i), r_send.at[i], r_recv.at[i], mate)

    for i, (first, n) in enumerate(CHUNKS):
        load(i).wait()
        if i + 2 < len(CHUNKS):
            load(i + 2).start()
        else:
            for c in range((i - 2) * 4, (i - 1) * 4):
                cache_copy(c).start()
        res = jnp.dot(u_ref[...], wbuf[:, first * HD:(first + n) * HD], preferred_element_type=F32)
        for h in range(n):
            tile = res[:, h * HD:(h + 1) * HD]
            if first + h < GRP + 1:
                tile = tile * cos_t + pltpu.roll(tile, HD // 2, 1) * sin_t
            ex[j, first + h] = tile
        to_side(i).start()
        to_mate(i).start()
    for i in range(len(CHUNKS)):
        to_side(i).wait_recv()
        relay(i).start()
    for i in range(len(CHUNKS)):
        to_mate(i).wait_recv()
        relay(i).wait_recv()
    for g in range(KVL):
        for r in range(GRP):
            q_ref[pl.ds(g * GRP + r, B, stride=ROWS), :] = ex[g, r]
        kn = ex[g, GRP]
        vn = ex[g, GRP + 1]
        for half in range(2):
            kn_ref[pl.ds(half * KVL + g, B, stride=8), :] = kn
            vn_ref[pl.ds(half * KVL + g, B, stride=8), :] = vn
    for i in range(len(CHUNKS)):
        to_side(i).wait_send()
        to_mate(i).wait_send()
        relay(i).wait_send()
    for i in range(8):
        cache_copy(i).wait()


PAIRS = B // 2


def attn_kernel(ctx_ref, q_ref, kn_ref, vn_ref, k_ref, v_ref, part_ref, kbuf, vbuf, ko_ref, vo_ref, bias, acc2, m2, l2, out_sem):
    base = lax.axis_index("kvp") * T

    def flush(i, which):
        src, dst = ((kbuf, ko_ref), (vbuf, vo_ref))[which]
        some = pl.ds(4 * i, 4)
        return pltpu.make_async_copy(src.at[some], dst.at[some], out_sem.at[which, i])

    row = lax.broadcasted_iota(jnp.int32, (2 * ROWS, KVL * T), 0)
    row = jnp.where(row >= ROWS, row - ROWS, row)
    col = lax.broadcasted_iota(jnp.int32, (2 * ROWS, KVL * T), 1)
    head = (row >= GRP).astype(jnp.int32) + (row >= 2 * GRP).astype(jnp.int32) + (row >= 3 * GRP).astype(jnp.int32)
    bias[...] = jnp.where(head == (col & (KVL - 1)), 0.0, NEG_FILL)
    first_half = lax.broadcasted_iota(jnp.int32, (2 * ROWS, 1), 0) < ROWS
    wrow = lax.broadcasted_iota(jnp.int32, (16, HD), 0)

    def patch(b):
        pos = ctx_ref[b] - base

        @pl.when((pos >= 0) & (pos < T))
        def _():
            win = pl.ds(pl.multiple_of((pos // 4) * 16, 16), 16)
            hit = (wrow // KVL) == (pos & 3)
            for new_ref, buf in ((kn_ref, kbuf), (vn_ref, vbuf)):
                new8 = new_ref[pl.ds(b * 8, 8), :]
                new16 = jnp.concatenate([new8, new8], axis=0)
                buf[b, win, :] = jnp.where(hit, new16, buf[b, win, :].astype(F32)).astype(BF16)

    def attend(p):
        b = 2 * p
        q = q_ref[pl.ds(p * 2 * ROWS, 2 * ROWS), :]
        lhs = jnp.concatenate([jnp.where(first_half, q, 0.0), jnp.where(first_half, 0.0, q)], axis=1).astype(BF16)
        keys = jnp.concatenate([kbuf[b], kbuf[b + 1]], axis=1)
        s = lax.dot_general(lhs, keys, (((1,), (1,)), ((), ())), preferred_element_type=F32)
        lim = jnp.where(first_half, (ctx_ref[b] - base + 1) * KVL, (ctx_ref[b + 1] - base + 1) * KVL)
        cols = lax.broadcasted_iota(jnp.int32, (2 * ROWS, KVL * T), 1)
        s = jnp.where(cols < lim, s * HD ** -0.5 + bias[...], NEG_FILL)
        m = jnp.max(s, axis=1, keepdims=True)
        w = jnp.exp(s - m)
        values = jnp.concatenate([vbuf[b], vbuf[b + 1]], axis=1)
        o = jnp.dot(w.astype(BF16), values, preferred_element_type=F32)
        rows = pl.ds(p * 2 * ROWS, 2 * ROWS)
        acc2[rows, :] = jnp.where(first_half, o[:, :HD], o[:, HD:])
        m2[rows, :] = jnp.broadcast_to(m, (2 * ROWS, HD))
        l2[rows, :] = jnp.broadcast_to(jnp.sum(w, axis=1, keepdims=True), (2 * ROWS, HD))

    @pl.loop(0, B // 4)
    def _(it):
        for k in range(4):
            patch(it * 4 + k)
        flush(it, 0).start()
        flush(it, 1).start()

    @pl.loop(0, PAIRS // 2)
    def _(it):
        for k in range(2):
            attend(it * 2 + k)

    lane = lax.broadcasted_iota(jnp.int32, (B, HD), 1)
    for g in range(KVL):
        stats = jnp.zeros((B, HD), F32)
        for r in range(GRP):
            rows = pl.ds(g * GRP + r, B, stride=ROWS)
            part_ref[g, r] = acc2[rows, :]
            stats = jnp.where(lane == r, m2[rows, :], stats)
            stats = jnp.where(lane == 8 + r, l2[rows, :], stats)
        part_ref[g, GRP] = stats

    @pl.loop(0, B // 4)
    def _(i):
        flush(i, 0).wait()
        flush(i, 1).wait()


NCH = 5
CW = D // NCH
GCH = 256
FLIP = 4
FLIPS = (4, 1, 3, 3, 1)


def tail_kernel(part_ref, x_hbm, g_hbm, wo_hbm, wg_hbm, wu_hbm, wd_hbm, out_ref,
                x_ref, g_ref, wo, w2, rx, attn, n_ref, y_ref, pbuf, sbuf, pair_a, pair_b, rs_a, rs_b, ag_a, ag_b,
                x_sem, w_sem, gu_sem, wd_sem, c_send, c_recv, d_send, d_recv, s_send, s_recv, a_send, a_recv, f_send, f_recv):
    t = lax.axis_index("tp")
    j = lax.axis_index("kvp")
    core = lax.rem(j, 2)
    xpos = j // 2
    quarter = t * 2 + xpos
    mate = {"tp": t, "kvp": j + 1 - 2 * core}
    chips = []
    for e in (1, 2, 3):
        tt = t if e == 1 else 1 - t
        xx = xpos if e == 2 else 1 - xpos
        chips.append(({"tp": tt, "kvp": xx * 2 + core}, tt * 2 + xx))
    ring = [{"tp": t, "kvp": lax.rem(j + d, 4)} for d in (1, 2, 3)]

    wo_copy = pltpu.make_async_copy(wo_hbm, wo, w_sem)
    wo_copy.start()
    x_copy = pltpu.make_async_copy(x_hbm, x_ref, x_sem.at[0])
    g_copy = pltpu.make_async_copy(g_hbm, g_ref, x_sem.at[1])
    x_copy.start()
    g_copy.start()
    enter(tuple(ring) + (chips[1][0], chips[2][0]))

    def combine_copy(d):
        return remote(part_ref.at[lax.rem(j + d, 4)], rx.at[d - 1], c_send.at[d - 1], c_recv.at[d - 1], ring[d - 1])

    for d in (2, 1, 3):
        combine_copy(d).start()

    full = FFL // GCH
    rest = FFL - full * GCH
    spans = [(i * GCH, GCH) for i in range(full)] + [(full * GCH, rest)]

    def gate_copy(i, which):
        first, n = spans[i]
        src = (wg_hbm, wu_hbm)[which]
        return pltpu.make_async_copy(src.at[pl.ds(first, n)], w2.at[which, pl.ds(first, n)], gu_sem.at[which, i])

    def down_copy(i):
        rows = pl.ds(*spans[i])
        return pltpu.make_async_copy(wd_hbm.at[rows], w2.at[0, rows], wd_sem.at[i])

    wo_copy.wait()
    x_copy.wait()
    g_copy.wait()
    for i in range(len(spans)):
        gate_copy(i, 0).start()
        gate_copy(i, 1).start()

    flipped = [0]

    def flip(blocks):
        for block in range(flipped[0], min(flipped[0] + blocks, 2 * full)):
            i, which = block // 2, block % 2
            gate_copy(i, which).wait()

            @pl.loop(0, D // (GCH * FLIP))
            def _(u):
                for v in range(FLIP):
                    rows = pl.ds(i * GCH, GCH)
                    cols = pl.ds(pl.multiple_of((u * FLIP + v) * GCH, GCH), GCH)
                    w2[which, rows, cols] = w2[which, rows, cols].T
        flipped[0] += blocks

    flip(FLIPS[0])
    for d in (1, 2, 3):
        combine_copy(d).wait_recv()
    stats = [part_ref[j, GRP]] + [rx[i, GRP] for i in range(3)]
    for r in range(GRP):
        ms = [s[:, r:r + 1] for s in stats]
        top = jnp.maximum(jnp.maximum(ms[0], ms[1]), jnp.maximum(ms[2], ms[3]))
        scales = [jnp.exp(m - top) for m in ms]
        denom = sum(sc * s[:, 8 + r:9 + r] for sc, s in zip(scales, stats))
        total = part_ref[j, r] * scales[0]
        for i in range(3):
            total = total + rx[i, r] * scales[i + 1]
        attn[:, r * HD:(r + 1) * HD] = (total / denom).astype(BF16)

    def all_sum(which, product, base, pair, rs, ag):
        def pair_copy(k):
            return remote(pbuf.at[k, pl.ds((1 - core) * 4, 4)], pair.at[k], d_send.at[which, k], d_recv.at[which, k], mate)

        def scatter_copy(k, e):
            dev, q = chips[e]
            return remote(sbuf.at[k, q], rs.at[k, e], s_send.at[which, k, e], s_recv.at[which, k, e], dev)

        own = core * 4 + quarter

        def gather_copy(k, e):
            dev = mate if e == 3 else chips[e][0]
            return remote(ag.at[k * 8 + own], ag.at[k * 8 + own], a_send.at[which, k, e], a_recv.at[which, k, e], dev)

        def forward_copy(k, e):
            slot = k * 8 + core * 4 + chips[e][1]
            return remote(ag.at[slot], ag.at[slot], f_send.at[which, k, e], f_recv.at[which, k, e], mate)

        for k in range(NCH):
            res = product(k)
            for i in range(8):
                pbuf[k, i] = res[:, i * HD:(i + 1) * HD]
            pair_copy(k).start()
        if which == 0:
            flip(FLIPS[1])
        for k in range(NCH):
            pair_copy(k).wait_recv()
            for i in range(4):
                sbuf[k, i] = pbuf[k, core * 4 + i] + pair[k, i]
            for e in (2, 0, 1):
                scatter_copy(k, e).start()
        if which == 0:
            flip(FLIPS[2])
        for k in range(NCH):
            for e in range(3):
                scatter_copy(k, e).wait_recv()
            total = sbuf[k, quarter] + rs[k, 0] + rs[k, 1] + rs[k, 2]
            ag[k * 8 + own] = (base(k * 8 + own) + total).astype(BF16).astype(F32)
            for e in (2, 0, 1, 3):
                gather_copy(k, e).start()
        if which == 0:
            flip(FLIPS[3])
        for k in range(NCH):
            for e in range(3):
                gather_copy(k, e).wait_recv()
                forward_copy(k, e).start()
        if which == 0:
            flip(FLIPS[4])
        for k in range(NCH):
            gather_copy(k, 3).wait_recv()
            for e in range(3):
                forward_copy(k, e).wait_recv()
        for k in range(NCH):
            pair_copy(k).wait_send()
            for e in range(3):
                scatter_copy(k, e).wait_send()
                forward_copy(k, e).wait_send()
            for e in range(4):
                gather_copy(k, e).wait_send()

    def o_product(k):
        return jnp.dot(attn[...], wo[:, k * CW:(k + 1) * CW], preferred_element_type=F32)

    def x_base(i):
        return x_ref[:, pl.ds(pl.multiple_of(i * HD, HD), HD)].astype(F32)

    all_sum(0, o_product, x_base, pair_a, rs_a, ag_a)

    squares = jnp.zeros((B, HD), F32)
    for i in range(D // HD):
        squares = squares + ag_a[i] * ag_a[i]
    inv = lax.rsqrt(jnp.sum(squares, axis=-1, keepdims=True) / D + EPS)
    for i in range(D // HD):
        n_ref[:, i * HD:(i + 1) * HD] = (ag_a[i] * inv * g_ref[i:i + 1, :].astype(F32)).astype(BF16)

    def act(gate, up):
        return (jax.nn.silu(gate) * up).astype(BF16)

    for i in range(full):
        rows = pl.ds(i * GCH, GCH)
        gate = up = None
        for k in range(D // GCH):
            cols = slice(k * GCH, (k + 1) * GCH)
            g_k = jnp.dot(n_ref[:, cols], w2[0, rows, cols], preferred_element_type=F32)
            u_k = jnp.dot(n_ref[:, cols], w2[1, rows, cols], preferred_element_type=F32)
            gate = g_k if gate is None else gate + g_k
            up = u_k if up is None else up + u_k
        y_ref[:, i * GCH:(i + 1) * GCH] = act(gate, up)
        down_copy(i).start()
    first, n = spans[full]
    gate_copy(full, 0).wait()
    gate_copy(full, 1).wait()
    dims = (((1,), (1,)), ((), ()))
    gate = lax.dot_general(n_ref[...], w2[0, pl.ds(first, n), :], dims, preferred_element_type=F32)
    up = lax.dot_general(n_ref[...], w2[1, pl.ds(first, n), :], dims, preferred_element_type=F32)
    y_ref[:, first:first + n] = act(gate, up)
    down_copy(full).start()
    for i in range(len(spans)):
        down_copy(i).wait()

    def down_product(k):
        return jnp.dot(y_ref[...], w2[0, :, k * CW:(k + 1) * CW], preferred_element_type=F32)

    all_sum(1, down_product, lambda i: ag_a[i], pair_b, rs_b, ag_b)
    for i in range(D // HD):
        out_ref[:, i * HD:(i + 1) * HD] = ag_b[i].astype(BF16)
    for d in (1, 2, 3):
        combine_copy(d).wait_send()


def vmem():
    return pl.BlockSpec(memory_space=pltpu.VMEM)


def hbm():
    return pl.BlockSpec(memory_space=pl.ANY)


def in_hbm(a):
    return pltpu.with_memory_space_constraint(a, pltpu.HBM)


def in_vmem(a):
    return pltpu.with_memory_space_constraint(a, pltpu.VMEM)


def smem():
    return pl.BlockSpec(memory_space=pltpu.SMEM)


def dma(*shape):
    return pltpu.SemaphoreType.DMA(shape)


def layer_step(x_in, ctx_len, g_attn, g_mlp, w_qkv, w_o, w_gate, w_up, w_down, k_cache, v_cache):
    freq = ROPE_THETA ** (-2.0 * np.arange(HD // 2, dtype=np.float64) / HD)
    freq = np.concatenate([freq, freq]).astype(np.float32).reshape(1, HD)
    kc = k_cache.reshape(B, T * KVL, HD)
    vc = v_cache.reshape(B, T * KVL, HD)
    nch = len(CHUNKS)
    q2, kn, vn, kc, vc = pl.pallas_call(
        qkv_kernel,
        out_shape=(pltpu.VMEM((B * ROWS, HD), F32), pltpu.VMEM((B * 8, HD), F32), pltpu.VMEM((B * 8, HD), F32),
                   pltpu.VMEM(kc.shape, BF16), pltpu.VMEM(vc.shape, BF16)),
        in_specs=[smem(), vmem(), hbm(), hbm(), hbm(), hbm(), hbm()],
        out_specs=(vmem(),) * 5,
        scratch_shapes=[
            pltpu.VMEM((B, D), BF16), pltpu.VMEM((D // HD, HD), BF16),
            pltpu.VMEM((D, QCOLS), BF16), pltpu.VMEM((B, D), BF16), pltpu.VMEM((KVL, GRP + 2, B, HD), F32),
            dma(2), dma(nch), dma(8), dma(nch), dma(nch), dma(nch), dma(nch), dma(nch), dma(nch),
        ],
        compiler_params=pltpu.CompilerParams(collective_id=0, has_side_effects=True, vmem_limit_bytes=MIB * 16),
        name="qkv",
    )(in_hbm(ctx_len), in_hbm(freq), in_hbm(x_in), in_hbm(g_attn.reshape(D // HD, HD)), in_hbm(w_qkv), in_hbm(kc), in_hbm(vc))

    part, kc, vc, k_out, v_out = pl.pallas_call(
        attn_kernel,
        out_shape=(pltpu.VMEM((KVL, GRP + 1, B, HD), F32), pltpu.VMEM(kc.shape, BF16), pltpu.VMEM(vc.shape, BF16),
                   jax.ShapeDtypeStruct(kc.shape, BF16), jax.ShapeDtypeStruct(vc.shape, BF16)),
        in_specs=[smem(), vmem(), vmem(), vmem(), vmem(), vmem()],
        out_specs=(vmem(), vmem(), vmem(), hbm(), hbm()),
        scratch_shapes=[
            pltpu.VMEM((2 * ROWS, KVL * T), F32),
            pltpu.VMEM((B * ROWS, HD), F32), pltpu.VMEM((B * ROWS, HD), F32), pltpu.VMEM((B * ROWS, HD), F32),
            dma(2, B // 4),
        ],
        input_output_aliases={4: 1, 5: 2},
        compiler_params=pltpu.CompilerParams(vmem_limit_bytes=MIB * 4),
        name="attn",
    )(in_hbm(ctx_len), q2, kn, vn, kc, vc)

    x_out = pl.pallas_call(
        tail_kernel,
        out_shape=pltpu.VMEM((B, D), BF16),
        in_specs=[vmem(), hbm(), hbm(), hbm(), hbm(), hbm(), hbm()],
        out_specs=vmem(),
        scratch_shapes=[
            pltpu.VMEM((B, D), BF16), pltpu.VMEM((D // HD, HD), BF16), pltpu.VMEM(w_o.shape, BF16), pltpu.VMEM((2, FFL, D), BF16),
            pltpu.VMEM((3, GRP + 1, B, HD), F32), pltpu.VMEM((B, GRP * HD), BF16), pltpu.VMEM((B, D), BF16), pltpu.VMEM((B, FFL), BF16),
            pltpu.VMEM((NCH, 8, B, HD), F32), pltpu.VMEM((NCH, 4, B, HD), F32),
            pltpu.VMEM((NCH, 4, B, HD), F32), pltpu.VMEM((NCH, 4, B, HD), F32),
            pltpu.VMEM((NCH, 3, B, HD), F32), pltpu.VMEM((NCH, 3, B, HD), F32),
            pltpu.VMEM((D // HD, B, HD), F32), pltpu.VMEM((D // HD, B, HD), F32),
            dma(2), pltpu.SemaphoreType.DMA, dma(2, 7), dma(7), dma(3), dma(3),
            dma(2, NCH), dma(2, NCH), dma(2, NCH, 3), dma(2, NCH, 3), dma(2, NCH, 4), dma(2, NCH, 4), dma(2, NCH, 3), dma(2, NCH, 3),
        ],
        compiler_params=pltpu.CompilerParams(collective_id=1, has_side_effects=True, vmem_limit_bytes=TAIL_VMEM),
        cost_estimate=pl.CostEstimate(flops=10 ** 10, bytes_accessed=10 ** 8, transcendentals=0),
        name="tail",
    )(in_vmem(part), in_hbm(x_in), in_hbm(g_mlp.reshape(D // HD, HD)), in_hbm(w_o), in_hbm(w_gate.T), in_hbm(w_up.T), in_hbm(w_down))
    return x_out, k_out.reshape(k_cache.shape), v_out.reshape(v_cache.shape)


def solution(mesh):
    x_spec = P("dp", None)
    cache_spec = P("dp", "kvp", "tp", None)
    model_axes = ("tp", "kvp")
    in_specs = (x_spec, P("dp"), P(None), P(None), P(None, "tp"), P(model_axes, None), P(None, model_axes), P(None, model_axes), P(model_axes, None), cache_spec, cache_spec)
    return jax.shard_map(layer_step, mesh=mesh, in_specs=in_specs, out_specs=(x_spec, cache_spec, cache_spec), check_vma=False)
```

```python
import jax
import jax.numpy as jnp
import numpy as np
from jax import lax
from jax.experimental import pallas as pl
from jax.experimental.pallas import tpu as pltpu
from jax.sharding import PartitionSpec as P

ROPE_THETA = 500000.0
EPS = 1e-5
NEG_FILL = -1e30
MESH = pl.DeviceIdType.MESH
F32 = jnp.float32
BF16 = jnp.bfloat16

D = 5120
HD = 128
B = 32
T = 256
KVL = 4
GRP = 5
ROWS = 24
QCOLS = (GRP + 2) * HD
FFL = 1728
MIB = 1024 * 1024
TAIL_VMEM = 56 * MIB


def remote(src, dst, send, recv, dev):
    return pltpu.make_async_remote_copy(src_ref=src, dst_ref=dst, send_sem=send, recv_sem=recv, device_id=dev, device_id_type=MESH)


def enter(peers):
    barrier = pltpu.get_barrier_semaphore()
    for peer in peers:
        pl.semaphore_signal(barrier, inc=1, device_id=peer, device_id_type=MESH)
    pl.semaphore_wait(barrier, len(peers))


CHUNKS = ((0, 2), (2, 2), (4, 2), (6, 1))


def qkv_kernel(ctx_ref, freq_ref, x_hbm, g_hbm, w_ref, k_hbm, v_hbm, q_ref, kn_ref, vn_ref, kc_ref, vc_ref,
               x_ref, g_ref, wbuf, u_ref, ex, x_sem, w_sem, c_sem, m_send, m_recv, x_send, x_recv, r_send, r_recv):
    j = lax.axis_index("kvp")
    mate = {"kvp": j + 1 - 2 * lax.rem(j, 2)}
    side = {"kvp": lax.rem(j + 2, 4)}
    x_copy = pltpu.make_async_copy(x_hbm, x_ref, x_sem.at[0])
    g_copy = pltpu.make_async_copy(g_hbm, g_ref, x_sem.at[1])
    x_copy.start()
    g_copy.start()

    def cache_copy(i):
        src, dst = ((k_hbm, kc_ref), (v_hbm, vc_ref))[i // 4]
        some = pl.ds((i % 4) * 8, 8)
        return pltpu.make_async_copy(src.at[some], dst.at[some], c_sem.at[i])

    def load(i):
        first, n = CHUNKS[i]
        cols = pl.ds(pl.multiple_of(j * QCOLS + first * HD, HD), n * HD)
        return pltpu.make_async_copy(w_ref.at[:, cols], wbuf.at[:, pl.ds(first * HD, n * HD)], w_sem.at[i])

    load(0).start()
    load(1).start()
    enter((mate, side))
    row = lax.broadcasted_iota(jnp.int32, (B, HD), 0)
    lane = lax.broadcasted_iota(jnp.int32, (B, HD), 1)
    ctx = jnp.zeros((B, HD), F32)
    for b in range(B):
        ctx = jnp.where(row == b, ctx_ref[b].astype(F32), ctx)
    angles = ctx * freq_ref[...]
    cos_t = jnp.cos(angles)
    sin_t = jnp.sin(angles)
    sin_t = jnp.where(lane < HD // 2, -sin_t, sin_t)
    x_copy.wait()
    g_copy.wait()
    squares = jnp.zeros((B, HD), F32)
    for i in range(D // HD):
        xf = x_ref[:, i * HD:(i + 1) * HD].astype(F32)
        squares = squares + xf * xf
    inv = lax.rsqrt(jnp.sum(squares, axis=-1, keepdims=True) / D + EPS)
    for i in range(D // HD):
        xf = x_ref[:, i * HD:(i + 1) * HD].astype(F32)
        u_ref[:, i * HD:(i + 1) * HD] = (xf * inv * g_ref[i:i + 1, :].astype(F32)).astype(BF16)
    q_ref[...] = jnp.zeros_like(q_ref)

    def piece(slot, i):
        first, n = CHUNKS[i]
        return ex.at[slot, pl.ds(first, n)]

    def to_mate(i):
        return remote(piece(j, i), piece(j, i), m_send.at[i], m_recv.at[i], mate)

    def to_side(i):
        return remote(piece(j, i), piece(j, i), x_send.at[i], x_recv.at[i], side)

    def relay(i):
        slot = lax.rem(j + 2, 4)
        return remote(piece(slot, i), piece(slot, i), r_send.at[i], r_recv.at[i], mate)

    for i, (first, n) in enumerate(CHUNKS):
        load(i).wait()
        if i + 2 < len(CHUNKS):
            load(i + 2).start()
        else:
            for c in range((i - 2) * 4, (i - 1) * 4):
                cache_copy(c).start()
        res = jnp.dot(u_ref[...], wbuf[:, first * HD:(first + n) * HD], preferred_element_type=F32)
        for h in range(n):
            tile = res[:, h * HD:(h + 1) * HD]
            if first + h < GRP + 1:
                tile = tile * cos_t + pltpu.roll(tile, HD // 2, 1) * sin_t
            ex[j, first + h] = tile
        to_side(i).start()
        to_mate(i).start()
    for i in range(len(CHUNKS)):
        to_side(i).wait_recv()
        relay(i).start()
    for i in range(len(CHUNKS)):
        to_mate(i).wait_recv()
        relay(i).wait_recv()
    for g in range(KVL):
        for r in range(GRP):
            q_ref[pl.ds(g * GRP + r, B, stride=ROWS), :] = ex[g, r]
        kn = ex[g, GRP]
        vn = ex[g, GRP + 1]
        for half in range(2):
            kn_ref[pl.ds(half * KVL + g, B, stride=8), :] = kn
            vn_ref[pl.ds(half * KVL + g, B, stride=8), :] = vn
    for i in range(len(CHUNKS)):
        to_side(i).wait_send()
        to_mate(i).wait_send()
        relay(i).wait_send()
    for i in range(8):
        cache_copy(i).wait()


PAIRS = B // 2


def attn_kernel(ctx_ref, q_ref, kn_ref, vn_ref, k_ref, v_ref, part_ref, kbuf, vbuf, ko_ref, vo_ref, bias, acc2, m2, l2, out_sem):
    base = lax.axis_index("kvp") * T

    def flush(i, which):
        src, dst = ((kbuf, ko_ref), (vbuf, vo_ref))[which]
        some = pl.ds(4 * i, 4)
        return pltpu.make_async_copy(src.at[some], dst.at[some], out_sem.at[which, i])

    row = lax.broadcasted_iota(jnp.int32, (2 * ROWS, KVL * T), 0)
    row = jnp.where(row >= ROWS, row - ROWS, row)
    col = lax.broadcasted_iota(jnp.int32, (2 * ROWS, KVL * T), 1)
    head = (row >= GRP).astype(jnp.int32) + (row >= 2 * GRP).astype(jnp.int32) + (row >= 3 * GRP).astype(jnp.int32)
    bias[...] = jnp.where(head == (col & (KVL - 1)), 0.0, NEG_FILL)
    first_half = lax.broadcasted_iota(jnp.int32, (2 * ROWS, 1), 0) < ROWS
    wrow = lax.broadcasted_iota(jnp.int32, (16, HD), 0)

    def patch(b):
        pos = ctx_ref[b] - base

        @pl.when((pos >= 0) & (pos < T))
        def _():
            win = pl.ds(pl.multiple_of((pos // 4) * 16, 16), 16)
            hit = (wrow // KVL) == (pos & 3)
            for new_ref, buf in ((kn_ref, kbuf), (vn_ref, vbuf)):
                new8 = new_ref[pl.ds(b * 8, 8), :]
                new16 = jnp.concatenate([new8, new8], axis=0)
                buf[b, win, :] = jnp.where(hit, new16, buf[b, win, :].astype(F32)).astype(BF16)

    def attend(p):
        b = 2 * p
        q = q_ref[pl.ds(p * 2 * ROWS, 2 * ROWS), :]
        lhs = jnp.concatenate([jnp.where(first_half, q, 0.0), jnp.where(first_half, 0.0, q)], axis=1).astype(BF16)
        keys = jnp.concatenate([kbuf[b], kbuf[b + 1]], axis=1)
        s = lax.dot_general(lhs, keys, (((1,), (1,)), ((), ())), preferred_element_type=F32)
        lim = jnp.where(first_half, (ctx_ref[b] - base + 1) * KVL, (ctx_ref[b + 1] - base + 1) * KVL)
        cols = lax.broadcasted_iota(jnp.int32, (2 * ROWS, KVL * T), 1)
        s = jnp.where(cols < lim, s * HD ** -0.5 + bias[...], NEG_FILL)
        m = jnp.max(s, axis=1, keepdims=True)
        w = jnp.exp(s - m)
        values = jnp.concatenate([vbuf[b], vbuf[b + 1]], axis=1)
        o = jnp.dot(w.astype(BF16), values, preferred_element_type=F32)
        rows = pl.ds(p * 2 * ROWS, 2 * ROWS)
        acc2[rows, :] = jnp.where(first_half, o[:, :HD], o[:, HD:])
        m2[rows, :] = jnp.broadcast_to(m, (2 * ROWS, HD))
        l2[rows, :] = jnp.broadcast_to(jnp.sum(w, axis=1, keepdims=True), (2 * ROWS, HD))

    @pl.loop(0, B // 4)
    def _(it):
        for k in range(4):
            patch(it * 4 + k)
        flush(it, 0).start()
        flush(it, 1).start()

    @pl.loop(0, PAIRS // 2)
    def _(it):
        for k in range(2):
            attend(it * 2 + k)

    lane = lax.broadcasted_iota(jnp.int32, (B, HD), 1)
    for g in range(KVL):
        stats = jnp.zeros((B, HD), F32)
        for r in range(GRP):
            rows = pl.ds(g * GRP + r, B, stride=ROWS)
            part_ref[g, r] = acc2[rows, :]
            stats = jnp.where(lane == r, m2[rows, :], stats)
            stats = jnp.where(lane == 8 + r, l2[rows, :], stats)
        part_ref[g, GRP] = stats

    @pl.loop(0, B // 4)
    def _(i):
        flush(i, 0).wait()
        flush(i, 1).wait()


NCH = 5
CW = D // NCH
GCH = 256
FLIP = 4
AHEAD = 3
FLIPS = (3, 1, 3, 3, 2)


def tail_kernel(part_ref, x_hbm, g_hbm, wo_hbm, wg_hbm, wu_hbm, wd_hbm, out_ref,
                x_ref, g_ref, wo, w2, rx, attn, n_ref, y_ref, pbuf, sbuf, pair_a, pair_b, rs_a, rs_b, ag_a, ag_b,
                x_sem, w_sem, gu_sem, wd_sem, c_send, c_recv, d_send, d_recv, s_send, s_recv, a_send, a_recv, f_send, f_recv):
    t = lax.axis_index("tp")
    j = lax.axis_index("kvp")
    core = lax.rem(j, 2)
    xpos = j // 2
    quarter = t * 2 + xpos
    mate = {"tp": t, "kvp": j + 1 - 2 * core}
    chips = []
    for e in (1, 2, 3):
        tt = t if e == 1 else 1 - t
        xx = xpos if e == 2 else 1 - xpos
        chips.append(({"tp": tt, "kvp": xx * 2 + core}, tt * 2 + xx))
    ring = [{"tp": t, "kvp": lax.rem(j + d, 4)} for d in (1, 2, 3)]

    wo_copy = pltpu.make_async_copy(wo_hbm, wo, w_sem)
    wo_copy.start()
    x_copy = pltpu.make_async_copy(x_hbm, x_ref, x_sem.at[0])
    g_copy = pltpu.make_async_copy(g_hbm, g_ref, x_sem.at[1])
    x_copy.start()
    g_copy.start()
    enter(tuple(ring) + (chips[1][0], chips[2][0]))

    def combine_copy(d):
        return remote(part_ref.at[lax.rem(j + d, 4)], rx.at[d - 1], c_send.at[d - 1], c_recv.at[d - 1], ring[d - 1])

    for d in (2, 1, 3):
        combine_copy(d).start()

    full = FFL // GCH
    rest = FFL - full * GCH
    spans = [(i * GCH, GCH) for i in range(full)] + [(full * GCH, rest)]

    def gate_copy(i, which):
        first, n = spans[i]
        src = (wg_hbm, wu_hbm)[which]
        return pltpu.make_async_copy(src.at[pl.ds(first, n)], w2.at[which, pl.ds(first, n)], gu_sem.at[which, i])

    def down_copy(i):
        rows = pl.ds(*spans[i])
        return pltpu.make_async_copy(wd_hbm.at[rows], w2.at[0, rows], wd_sem.at[i])

    wo_copy.wait()
    x_copy.wait()
    g_copy.wait()
    order = [(i, which) for i in range(len(spans)) for which in range(2)]
    for block in range(AHEAD):
        gate_copy(*order[block]).start()

    flipped = [0]

    def flip(blocks):
        for block in range(flipped[0], min(flipped[0] + blocks, 2 * full)):
            i, which = block // 2, block % 2
            gate_copy(i, which).wait()
            if block + AHEAD < len(order):
                gate_copy(*order[block + AHEAD]).start()

            @pl.loop(0, D // (GCH * FLIP))
            def _(u):
                for v in range(FLIP):
                    rows = pl.ds(i * GCH, GCH)
                    cols = pl.ds(pl.multiple_of((u * FLIP + v) * GCH, GCH), GCH)
                    w2[which, rows, cols] = w2[which, rows, cols].T
        flipped[0] += blocks

    flip(FLIPS[0])
    for d in (1, 2, 3):
        combine_copy(d).wait_recv()
    stats = [part_ref[j, GRP]] + [rx[i, GRP] for i in range(3)]
    for r in range(GRP):
        ms = [s[:, r:r + 1] for s in stats]
        top = jnp.maximum(jnp.maximum(ms[0], ms[1]), jnp.maximum(ms[2], ms[3]))
        scales = [jnp.exp(m - top) for m in ms]
        denom = sum(sc * s[:, 8 + r:9 + r] for sc, s in zip(scales, stats))
        total = part_ref[j, r] * scales[0]
        for i in range(3):
            total = total + rx[i, r] * scales[i + 1]
        attn[:, r * HD:(r + 1) * HD] = (total / denom).astype(BF16)

    def all_sum(which, product, base, pair, rs, ag):
        def pair_copy(k):
            return remote(pbuf.at[k, pl.ds((1 - core) * 4, 4)], pair.at[k], d_send.at[which, k], d_recv.at[which, k], mate)

        def scatter_copy(k, e):
            dev, q = chips[e]
            return remote(sbuf.at[k, q], rs.at[k, e], s_send.at[which, k, e], s_recv.at[which, k, e], dev)

        own = core * 4 + quarter

        def gather_copy(k, e):
            dev = mate if e == 3 else chips[e][0]
            return remote(ag.at[k * 8 + own], ag.at[k * 8 + own], a_send.at[which, k, e], a_recv.at[which, k, e], dev)

        def forward_copy(k, e):
            slot = k * 8 + core * 4 + chips[e][1]
            return remote(ag.at[slot], ag.at[slot], f_send.at[which, k, e], f_recv.at[which, k, e], mate)

        for k in range(NCH):
            res = product(k)
            for i in range(8):
                pbuf[k, i] = res[:, i * HD:(i + 1) * HD]
            pair_copy(k).start()
        if which == 0:
            flip(FLIPS[1])
        for k in range(NCH):
            pair_copy(k).wait_recv()
            for i in range(4):
                sbuf[k, i] = pbuf[k, core * 4 + i] + pair[k, i]
            for e in (2, 0, 1):
                scatter_copy(k, e).start()
        if which == 0:
            flip(FLIPS[2])
        for k in range(NCH):
            for e in range(3):
                scatter_copy(k, e).wait_recv()
            total = sbuf[k, quarter] + rs[k, 0] + rs[k, 1] + rs[k, 2]
            ag[k * 8 + own] = (base(k * 8 + own) + total).astype(BF16).astype(F32)
            for e in (2, 0, 1, 3):
                gather_copy(k, e).start()
        if which == 0:
            flip(FLIPS[3])
        for k in range(NCH):
            for e in range(3):
                gather_copy(k, e).wait_recv()
                forward_copy(k, e).start()
        if which == 0:
            flip(FLIPS[4])
        for k in range(NCH):
            gather_copy(k, 3).wait_recv()
            for e in range(3):
                forward_copy(k, e).wait_recv()
        for k in range(NCH):
            pair_copy(k).wait_send()
            for e in range(3):
                scatter_copy(k, e).wait_send()
                forward_copy(k, e).wait_send()
            for e in range(4):
                gather_copy(k, e).wait_send()

    def o_product(k):
        return jnp.dot(attn[...], wo[:, k * CW:(k + 1) * CW], preferred_element_type=F32)

    def x_base(i):
        return x_ref[:, pl.ds(pl.multiple_of(i * HD, HD), HD)].astype(F32)

    all_sum(0, o_product, x_base, pair_a, rs_a, ag_a)

    squares = jnp.zeros((B, HD), F32)
    for i in range(D // HD):
        squares = squares + ag_a[i] * ag_a[i]
    inv = lax.rsqrt(jnp.sum(squares, axis=-1, keepdims=True) / D + EPS)
    for i in range(D // HD):
        n_ref[:, i * HD:(i + 1) * HD] = (ag_a[i] * inv * g_ref[i:i + 1, :].astype(F32)).astype(BF16)

    def act(gate, up):
        return (jax.nn.silu(gate) * up).astype(BF16)

    for i in range(full):
        rows = pl.ds(i * GCH, GCH)
        gate = up = None
        for k in range(D // GCH):
            cols = slice(k * GCH, (k + 1) * GCH)
            g_k = jnp.dot(n_ref[:, cols], w2[0, rows, cols], preferred_element_type=F32)
            u_k = jnp.dot(n_ref[:, cols], w2[1, rows, cols], preferred_element_type=F32)
            gate = g_k if gate is None else gate + g_k
            up = u_k if up is None else up + u_k
        y_ref[:, i * GCH:(i + 1) * GCH] = act(gate, up)
        down_copy(i).start()
    first, n = spans[full]
    gate_copy(full, 0).wait()
    gate_copy(full, 1).wait()
    dims = (((1,), (1,)), ((), ()))
    gate = lax.dot_general(n_ref[...], w2[0, pl.ds(first, n), :], dims, preferred_element_type=F32)
    up = lax.dot_general(n_ref[...], w2[1, pl.ds(first, n), :], dims, preferred_element_type=F32)
    y_ref[:, first:first + n] = act(gate, up)
    down_copy(full).start()
    for i in range(len(spans)):
        down_copy(i).wait()

    def down_product(k):
        return jnp.dot(y_ref[...], w2[0, :, k * CW:(k + 1) * CW], preferred_element_type=F32)

    all_sum(1, down_product, lambda i: ag_a[i], pair_b, rs_b, ag_b)
    for i in range(D // HD):
        out_ref[:, i * HD:(i + 1) * HD] = ag_b[i].astype(BF16)
    for d in (1, 2, 3):
        combine_copy(d).wait_send()


def vmem():
    return pl.BlockSpec(memory_space=pltpu.VMEM)


def hbm():
    return pl.BlockSpec(memory_space=pl.ANY)


def in_hbm(a):
    return pltpu.with_memory_space_constraint(a, pltpu.HBM)


def in_vmem(a):
    return pltpu.with_memory_space_constraint(a, pltpu.VMEM)


def smem():
    return pl.BlockSpec(memory_space=pltpu.SMEM)


def dma(*shape):
    return pltpu.SemaphoreType.DMA(shape)


def layer_step(x_in, ctx_len, g_attn, g_mlp, w_qkv, w_o, w_gate, w_up, w_down, k_cache, v_cache):
    freq = ROPE_THETA ** (-2.0 * np.arange(HD // 2, dtype=np.float64) / HD)
    freq = np.concatenate([freq, freq]).astype(np.float32).reshape(1, HD)
    kc = k_cache.reshape(B, T * KVL, HD)
    vc = v_cache.reshape(B, T * KVL, HD)
    nch = len(CHUNKS)
    q2, kn, vn, kc, vc = pl.pallas_call(
        qkv_kernel,
        out_shape=(pltpu.VMEM((B * ROWS, HD), F32), pltpu.VMEM((B * 8, HD), F32), pltpu.VMEM((B * 8, HD), F32),
                   pltpu.VMEM(kc.shape, BF16), pltpu.VMEM(vc.shape, BF16)),
        in_specs=[smem(), vmem(), hbm(), hbm(), hbm(), hbm(), hbm()],
        out_specs=(vmem(),) * 5,
        scratch_shapes=[
            pltpu.VMEM((B, D), BF16), pltpu.VMEM((D // HD, HD), BF16),
            pltpu.VMEM((D, QCOLS), BF16), pltpu.VMEM((B, D), BF16), pltpu.VMEM((KVL, GRP + 2, B, HD), F32),
            dma(2), dma(nch), dma(8), dma(nch), dma(nch), dma(nch), dma(nch), dma(nch), dma(nch),
        ],
        compiler_params=pltpu.CompilerParams(collective_id=0, has_side_effects=True, vmem_limit_bytes=MIB * 16),
        name="qkv",
    )(in_hbm(ctx_len), in_hbm(freq), in_hbm(x_in), in_hbm(g_attn.reshape(D // HD, HD)), in_hbm(w_qkv), in_hbm(kc), in_hbm(vc))

    part, kc, vc, k_out, v_out = pl.pallas_call(
        attn_kernel,
        out_shape=(pltpu.VMEM((KVL, GRP + 1, B, HD), F32), pltpu.VMEM(kc.shape, BF16), pltpu.VMEM(vc.shape, BF16),
                   jax.ShapeDtypeStruct(kc.shape, BF16), jax.ShapeDtypeStruct(vc.shape, BF16)),
        in_specs=[smem(), vmem(), vmem(), vmem(), vmem(), vmem()],
        out_specs=(vmem(), vmem(), vmem(), hbm(), hbm()),
        scratch_shapes=[
            pltpu.VMEM((2 * ROWS, KVL * T), F32),
            pltpu.VMEM((B * ROWS, HD), F32), pltpu.VMEM((B * ROWS, HD), F32), pltpu.VMEM((B * ROWS, HD), F32),
            dma(2, B // 4),
        ],
        input_output_aliases={4: 1, 5: 2},
        compiler_params=pltpu.CompilerParams(vmem_limit_bytes=MIB * 4),
        name="attn",
    )(in_hbm(ctx_len), q2, kn, vn, kc, vc)

    x_out = pl.pallas_call(
        tail_kernel,
        out_shape=pltpu.VMEM((B, D), BF16),
        in_specs=[vmem(), hbm(), hbm(), hbm(), hbm(), hbm(), hbm()],
        out_specs=vmem(),
        scratch_shapes=[
            pltpu.VMEM((B, D), BF16), pltpu.VMEM((D // HD, HD), BF16), pltpu.VMEM(w_o.shape, BF16), pltpu.VMEM((2, FFL, D), BF16),
            pltpu.VMEM((3, GRP + 1, B, HD), F32), pltpu.VMEM((B, GRP * HD), BF16), pltpu.VMEM((B, D), BF16), pltpu.VMEM((B, FFL), BF16),
            pltpu.VMEM((NCH, 8, B, HD), F32), pltpu.VMEM((NCH, 4, B, HD), F32),
            pltpu.VMEM((NCH, 4, B, HD), F32), pltpu.VMEM((NCH, 4, B, HD), F32),
            pltpu.VMEM((NCH, 3, B, HD), F32), pltpu.VMEM((NCH, 3, B, HD), F32),
            pltpu.VMEM((D // HD, B, HD), F32), pltpu.VMEM((D // HD, B, HD), F32),
            dma(2), pltpu.SemaphoreType.DMA, dma(2, 7), dma(7), dma(3), dma(3),
            dma(2, NCH), dma(2, NCH), dma(2, NCH, 3), dma(2, NCH, 3), dma(2, NCH, 4), dma(2, NCH, 4), dma(2, NCH, 3), dma(2, NCH, 3),
        ],
        compiler_params=pltpu.CompilerParams(collective_id=1, has_side_effects=True, vmem_limit_bytes=TAIL_VMEM),
        cost_estimate=pl.CostEstimate(flops=10 ** 10, bytes_accessed=10 ** 8, transcendentals=0),
        name="tail",
    )(in_vmem(part), in_hbm(x_in), in_hbm(g_mlp.reshape(D // HD, HD)), in_hbm(w_o), in_hbm(w_gate.T), in_hbm(w_up.T), in_hbm(w_down))
    return x_out, k_out.reshape(k_cache.shape), v_out.reshape(v_cache.shape)


def solution(mesh):
    x_spec = P("dp", None)
    cache_spec = P("dp", "kvp", "tp", None)
    model_axes = ("tp", "kvp")
    in_specs = (x_spec, P("dp"), P(None), P(None), P(None, "tp"), P(model_axes, None), P(None, model_axes), P(None, model_axes), P(model_axes, None), cache_spec, cache_spec)
    return jax.shard_map(layer_step, mesh=mesh, in_specs=in_specs, out_specs=(x_spec, cache_spec, cache_spec), check_vma=False)
```

```python
import jax
import jax.numpy as jnp
import numpy as np
from jax import lax
from jax.experimental import pallas as pl
from jax.experimental.pallas import tpu as pltpu
from jax.sharding import PartitionSpec as P

ROPE_THETA = 500000.0
EPS = 1e-5
NEG_FILL = -1e30
MESH = pl.DeviceIdType.MESH
F32 = jnp.float32
BF16 = jnp.bfloat16

D = 5120
HD = 128
B = 32
T = 256
KVL = 4
GRP = 5
ROWS = 24
QCOLS = (GRP + 2) * HD
FFL = 1728
MIB = 1024 * 1024
TAIL_VMEM = 56 * MIB


def remote(src, dst, send, recv, dev):
    return pltpu.make_async_remote_copy(src_ref=src, dst_ref=dst, send_sem=send, recv_sem=recv, device_id=dev, device_id_type=MESH)


def enter(peers):
    barrier = pltpu.get_barrier_semaphore()
    for peer in peers:
        pl.semaphore_signal(barrier, inc=1, device_id=peer, device_id_type=MESH)
    pl.semaphore_wait(barrier, len(peers))


WPARTS = 4
CPARTS = 8
FLIGHT = 6
CHUNKS = ((0, 2), (2, 2), (4, 2), (6, 1))


def qkv_kernel(ctx_ref, freq_ref, x_hbm, g_hbm, w_ref, k_hbm, v_hbm, q_ref, kn_ref, vn_ref, kc_ref, vc_ref,
               x_ref, g_ref, wbuf, u_ref, ex, x_sem, w_sem, m_send, m_recv, x_send, x_recv, r_send, r_recv):
    j = lax.axis_index("kvp")
    mate = {"kvp": j + 1 - 2 * lax.rem(j, 2)}
    side = {"kvp": lax.rem(j + 2, 4)}
    x_copy = pltpu.make_async_copy(x_hbm, x_ref, x_sem.at[0])
    g_copy = pltpu.make_async_copy(g_hbm, g_ref, x_sem.at[1])
    x_copy.start()
    g_copy.start()

    pieces = []
    last_piece = []
    for first, n in CHUNKS:
        depth = D * 2 // (WPARTS * n)
        for part in range(D // depth):
            rows = pl.ds(part * depth, depth)
            cols = pl.ds(pl.multiple_of(j * QCOLS + first * HD, HD), n * HD)
            pieces.append((w_ref.at[rows, cols], wbuf.at[rows, pl.ds(first * HD, n * HD)]))
        last_piece.append(len(pieces))
    n_weight = len(pieces)
    for i in range(2 * CPARTS):
        src, dst = ((k_hbm, kc_ref), (v_hbm, vc_ref))[i // CPARTS]
        some = pl.ds((i % CPARTS) * (B // CPARTS), B // CPARTS)
        pieces.append((src.at[some], dst.at[some]))

    def fetch(i):
        return pltpu.make_async_copy(*pieces[i], w_sem.at[i])

    for i in range(FLIGHT):
        fetch(i).start()
    enter((mate, side))
    row = lax.broadcasted_iota(jnp.int32, (B, HD), 0)
    lane = lax.broadcasted_iota(jnp.int32, (B, HD), 1)
    ctx = jnp.zeros((B, HD), F32)
    for b in range(B):
        ctx = jnp.where(row == b, ctx_ref[b].astype(F32), ctx)
    angles = ctx * freq_ref[...]
    cos_t = jnp.cos(angles)
    sin_t = jnp.sin(angles)
    sin_t = jnp.where(lane < HD // 2, -sin_t, sin_t)
    x_copy.wait()
    g_copy.wait()
    squares = jnp.zeros((B, HD), F32)
    for i in range(D // HD):
        xf = x_ref[:, i * HD:(i + 1) * HD].astype(F32)
        squares = squares + xf * xf
    inv = lax.rsqrt(jnp.sum(squares, axis=-1, keepdims=True) / D + EPS)
    for i in range(D // HD):
        xf = x_ref[:, i * HD:(i + 1) * HD].astype(F32)
        u_ref[:, i * HD:(i + 1) * HD] = (xf * inv * g_ref[i:i + 1, :].astype(F32)).astype(BF16)
    q_ref[...] = jnp.zeros_like(q_ref)

    def piece(slot, i):
        first, n = CHUNKS[i]
        return ex.at[slot, pl.ds(first, n)]

    def to_mate(i):
        return remote(piece(j, i), piece(j, i), m_send.at[i], m_recv.at[i], mate)

    def to_side(i):
        return remote(piece(j, i), piece(j, i), x_send.at[i], x_recv.at[i], side)

    def relay(i):
        slot = lax.rem(j + 2, 4)
        return remote(piece(slot, i), piece(slot, i), r_send.at[i], r_recv.at[i], mate)

    for i, (first, n) in enumerate(CHUNKS):
        for p in range(last_piece[i - 1] if i else 0, last_piece[i]):
            fetch(p).wait()
            fetch(p + FLIGHT).start()
        if i == len(CHUNKS) - 1:
            for p in range(n_weight + FLIGHT, len(pieces)):
                fetch(p).start()
        res = jnp.dot(u_ref[...], wbuf[:, first * HD:(first + n) * HD], preferred_element_type=F32)
        for h in range(n):
            tile = res[:, h * HD:(h + 1) * HD]
            if first + h < GRP + 1:
                tile = tile * cos_t + pltpu.roll(tile, HD // 2, 1) * sin_t
            ex[j, first + h] = tile
        to_side(i).start()
        to_mate(i).start()
    for i in range(len(CHUNKS)):
        to_side(i).wait_recv()
        relay(i).start()
    for i in range(len(CHUNKS)):
        to_mate(i).wait_recv()
        relay(i).wait_recv()
    for g in range(KVL):
        for r in range(GRP):
            q_ref[pl.ds(g * GRP + r, B, stride=ROWS), :] = ex[g, r]
        kn = ex[g, GRP]
        vn = ex[g, GRP + 1]
        for half in range(2):
            kn_ref[pl.ds(half * KVL + g, B, stride=8), :] = kn
            vn_ref[pl.ds(half * KVL + g, B, stride=8), :] = vn
    for i in range(len(CHUNKS)):
        to_side(i).wait_send()
        to_mate(i).wait_send()
        relay(i).wait_send()
    for i in range(n_weight, len(pieces)):
        fetch(i).wait()


PAIRS = B // 2


def attn_kernel(ctx_ref, q_ref, kn_ref, vn_ref, k_ref, v_ref, part_ref, kbuf, vbuf, ko_ref, vo_ref, bias, acc2, m2, l2, out_sem):
    base = lax.axis_index("kvp") * T

    def flush(i, which):
        src, dst = ((kbuf, ko_ref), (vbuf, vo_ref))[which]
        some = pl.ds(4 * i, 4)
        return pltpu.make_async_copy(src.at[some], dst.at[some], out_sem.at[which, i])

    row = lax.broadcasted_iota(jnp.int32, (2 * ROWS, KVL * T), 0)
    row = jnp.where(row >= ROWS, row - ROWS, row)
    col = lax.broadcasted_iota(jnp.int32, (2 * ROWS, KVL * T), 1)
    head = (row >= GRP).astype(jnp.int32) + (row >= 2 * GRP).astype(jnp.int32) + (row >= 3 * GRP).astype(jnp.int32)
    bias[...] = jnp.where(head == (col & (KVL - 1)), 0.0, NEG_FILL)
    first_half = lax.broadcasted_iota(jnp.int32, (2 * ROWS, 1), 0) < ROWS
    wrow = lax.broadcasted_iota(jnp.int32, (16, HD), 0)

    def patch(b):
        pos = ctx_ref[b] - base
        here = (pos >= 0) & (pos < T)
        pos = jnp.clip(pos, 0, T - 1)
        win = pl.ds(pl.multiple_of((pos // 4) * 16, 16), 16)
        hit = (wrow // KVL) == jnp.where(here, pos & 3, 4)
        for new_ref, buf in ((kn_ref, kbuf), (vn_ref, vbuf)):
            new8 = new_ref[pl.ds(b * 8, 8), :]
            new16 = jnp.concatenate([new8, new8], axis=0)
            buf[b, win, :] = jnp.where(hit, new16, buf[b, win, :].astype(F32)).astype(BF16)

    def attend(p):
        b = 2 * p
        q = q_ref[pl.ds(p * 2 * ROWS, 2 * ROWS), :]
        lhs = jnp.concatenate([jnp.where(first_half, q, 0.0), jnp.where(first_half, 0.0, q)], axis=1).astype(BF16)
        keys = jnp.concatenate([kbuf[b], kbuf[b + 1]], axis=1)
        s = lax.dot_general(lhs, keys, (((1,), (1,)), ((), ())), preferred_element_type=F32)
        lim = jnp.where(first_half, (ctx_ref[b] - base + 1) * KVL, (ctx_ref[b + 1] - base + 1) * KVL)
        cols = lax.broadcasted_iota(jnp.int32, (2 * ROWS, KVL * T), 1)
        s = jnp.where(cols < lim, s * HD ** -0.5 + bias[...], NEG_FILL)
        m = jnp.max(s, axis=1, keepdims=True)
        w = jnp.exp(s - m)
        values = jnp.concatenate([vbuf[b], vbuf[b + 1]], axis=1)
        o = jnp.dot(w.astype(BF16), values, preferred_element_type=F32)
        rows = pl.ds(p * 2 * ROWS, 2 * ROWS)
        acc2[rows, :] = jnp.where(first_half, o[:, :HD], o[:, HD:])
        m2[rows, :] = jnp.broadcast_to(m, (2 * ROWS, HD))
        l2[rows, :] = jnp.broadcast_to(jnp.sum(w, axis=1, keepdims=True), (2 * ROWS, HD))

    @pl.loop(0, B // 4)
    def _(it):
        for k in range(4):
            patch(it * 4 + k)
        flush(it, 0).start()
        flush(it, 1).start()

    @pl.loop(0, PAIRS // 4)
    def _(it):
        for k in range(4):
            attend(it * 4 + k)

    lane = lax.broadcasted_iota(jnp.int32, (B, HD), 1)
    for g in range(KVL):
        stats = jnp.zeros((B, HD), F32)
        for r in range(GRP):
            rows = pl.ds(g * GRP + r, B, stride=ROWS)
            part_ref[g, r] = acc2[rows, :]
            stats = jnp.where(lane == r, m2[rows, :], stats)
            stats = jnp.where(lane == 8 + r, l2[rows, :], stats)
        part_ref[g, GRP] = stats

    @pl.loop(0, B // 4)
    def _(i):
        flush(i, 0).wait()
        flush(i, 1).wait()


NCH = 5
CW = D // NCH
GCH = 256


def tail_kernel(part_ref, x_hbm, g_hbm, wo_hbm, wg_hbm, wu_hbm, wd_hbm, out_ref,
                x_ref, g_ref, wo, wg, wu, rx, attn, n_ref, y_ref, pbuf, sbuf, pair_a, pair_b, rs_a, rs_b, ag_a, ag_b,
                x_sem, w_sem, gu_sem, wd_sem, c_send, c_recv, d_send, d_recv, s_send, s_recv, a_send, a_recv, f_send, f_recv):
    t = lax.axis_index("tp")
    j = lax.axis_index("kvp")
    core = lax.rem(j, 2)
    xpos = j // 2
    quarter = t * 2 + xpos
    mate = {"tp": t, "kvp": j + 1 - 2 * core}
    chips = []
    for e in (1, 2, 3):
        tt = t if e == 1 else 1 - t
        xx = xpos if e == 2 else 1 - xpos
        chips.append(({"tp": tt, "kvp": xx * 2 + core}, tt * 2 + xx))
    ring = [{"tp": t, "kvp": lax.rem(j + d, 4)} for d in (1, 2, 3)]

    wo_copy = pltpu.make_async_copy(wo_hbm, wo, w_sem)
    wo_copy.start()
    x_copy = pltpu.make_async_copy(x_hbm, x_ref, x_sem.at[0])
    g_copy = pltpu.make_async_copy(g_hbm, g_ref, x_sem.at[1])
    x_copy.start()
    g_copy.start()
    enter(tuple(ring) + (chips[1][0], chips[2][0]))

    def combine_copy(d):
        return remote(part_ref.at[lax.rem(j + d, 4)], rx.at[d - 1], c_send.at[d - 1], c_recv.at[d - 1], ring[d - 1])

    for d in (2, 1, 3):
        combine_copy(d).start()

    full = FFL // GCH
    rest = FFL - full * GCH
    spans = [(i * GCH, GCH) for i in range(full)] + [(full * GCH, rest)]

    def gate_copy(i, which):
        first, n = spans[i]
        src, dst = ((wg_hbm, wg), (wu_hbm, wu))[which]
        return pltpu.make_async_copy(src.at[pl.ds(first, n)], dst.at[pl.ds(first, n)], gu_sem.at[which, i])

    def down_copy(i):
        rows = pl.ds(*spans[i])
        return pltpu.make_async_copy(wd_hbm.at[rows], wg.at[rows], wd_sem.at[i])

    wo_copy.wait()
    x_copy.wait()
    g_copy.wait()
    for i in range(len(spans)):
        gate_copy(i, 0).start()
        gate_copy(i, 1).start()

    for d in (1, 2, 3):
        combine_copy(d).wait_recv()
    stats = [part_ref[j, GRP]] + [rx[i, GRP] for i in range(3)]
    for r in range(GRP):
        ms = [s[:, r:r + 1] for s in stats]
        top = jnp.maximum(jnp.maximum(ms[0], ms[1]), jnp.maximum(ms[2], ms[3]))
        scales = [jnp.exp(m - top) for m in ms]
        denom = sum(sc * s[:, 8 + r:9 + r] for sc, s in zip(scales, stats))
        total = part_ref[j, r] * scales[0]
        for i in range(3):
            total = total + rx[i, r] * scales[i + 1]
        attn[:, r * HD:(r + 1) * HD] = (total / denom).astype(BF16)

    def all_sum(which, product, base, pair, rs, ag):
        def pair_copy(k):
            return remote(pbuf.at[k, pl.ds((1 - core) * 4, 4)], pair.at[k], d_send.at[which, k], d_recv.at[which, k], mate)

        def scatter_copy(k, e):
            dev, q = chips[e]
            return remote(sbuf.at[k, q], rs.at[k, e], s_send.at[which, k, e], s_recv.at[which, k, e], dev)

        own = core * 4 + quarter

        def gather_copy(k, e):
            dev = mate if e == 3 else chips[e][0]
            return remote(ag.at[k * 8 + own], ag.at[k * 8 + own], a_send.at[which, k, e], a_recv.at[which, k, e], dev)

        def forward_copy(k, e):
            slot = k * 8 + core * 4 + chips[e][1]
            return remote(ag.at[slot], ag.at[slot], f_send.at[which, k, e], f_recv.at[which, k, e], mate)

        for k in range(NCH):
            res = product(k)
            for i in range(8):
                pbuf[k, i] = res[:, i * HD:(i + 1) * HD]
            pair_copy(k).start()
        for k in range(NCH):
            pair_copy(k).wait_recv()
            for i in range(4):
                sbuf[k, i] = pbuf[k, core * 4 + i] + pair[k, i]
            for e in (2, 0, 1):
                scatter_copy(k, e).start()
        for k in range(NCH):
            for e in range(3):
                scatter_copy(k, e).wait_recv()
            total = sbuf[k, quarter] + rs[k, 0] + rs[k, 1] + rs[k, 2]
            ag[k * 8 + own] = (base(k * 8 + own) + total).astype(BF16).astype(F32)
            for e in (2, 0, 1, 3):
                gather_copy(k, e).start()
        for k in range(NCH):
            for e in range(3):
                gather_copy(k, e).wait_recv()
                forward_copy(k, e).start()
        for k in range(NCH):
            gather_copy(k, 3).wait_recv()
            for e in range(3):
                forward_copy(k, e).wait_recv()
        for k in range(NCH):
            pair_copy(k).wait_send()
            for e in range(3):
                scatter_copy(k, e).wait_send()
                forward_copy(k, e).wait_send()
            for e in range(4):
                gather_copy(k, e).wait_send()

    def o_product(k):
        return jnp.dot(attn[...], wo[:, k * CW:(k + 1) * CW], preferred_element_type=F32)

    def x_base(i):
        return x_ref[:, pl.ds(pl.multiple_of(i * HD, HD), HD)].astype(F32)

    all_sum(0, o_product, x_base, pair_a, rs_a, ag_a)

    squares = jnp.zeros((B, HD), F32)
    for i in range(D // HD):
        squares = squares + ag_a[i] * ag_a[i]
    inv = lax.rsqrt(jnp.sum(squares, axis=-1, keepdims=True) / D + EPS)
    for i in range(D // HD):
        n_ref[:, i * HD:(i + 1) * HD] = (ag_a[i] * inv * g_ref[i:i + 1, :].astype(F32)).astype(BF16)

    def gate_step(first, n):
        dims = (((1,), (1,)), ((), ()))
        gate = lax.dot_general(n_ref[...], wg[pl.ds(first, n), :], dims, preferred_element_type=F32)
        up = lax.dot_general(n_ref[...], wu[pl.ds(first, n), :], dims, preferred_element_type=F32)
        return (jax.nn.silu(gate) * up).astype(BF16)

    for i, (first, n) in enumerate(spans):
        gate_copy(i, 0).wait()
        gate_copy(i, 1).wait()
        y_ref[:, first:first + n] = gate_step(first, n)
        down_copy(i).start()
    for i in range(len(spans)):
        down_copy(i).wait()

    def down_product(k):
        return jnp.dot(y_ref[...], wg[:, k * CW:(k + 1) * CW], preferred_element_type=F32)

    all_sum(1, down_product, lambda i: ag_a[i], pair_b, rs_b, ag_b)
    for i in range(D // HD):
        out_ref[:, i * HD:(i + 1) * HD] = ag_b[i].astype(BF16)
    for d in (1, 2, 3):
        combine_copy(d).wait_send()


def vmem():
    return pl.BlockSpec(memory_space=pltpu.VMEM)


def hbm():
    return pl.BlockSpec(memory_space=pl.ANY)


def in_hbm(a):
    return pltpu.with_memory_space_constraint(a, pltpu.HBM)


def in_vmem(a):
    return pltpu.with_memory_space_constraint(a, pltpu.VMEM)


def smem():
    return pl.BlockSpec(memory_space=pltpu.SMEM)


def dma(*shape):
    return pltpu.SemaphoreType.DMA(shape)


def layer_step(x_in, ctx_len, g_attn, g_mlp, w_qkv, w_o, w_gate, w_up, w_down, k_cache, v_cache):
    freq = ROPE_THETA ** (-2.0 * np.arange(HD // 2, dtype=np.float64) / HD)
    freq = np.concatenate([freq, freq]).astype(np.float32).reshape(1, HD)
    kc = k_cache.reshape(B, T * KVL, HD)
    vc = v_cache.reshape(B, T * KVL, HD)
    nch = len(CHUNKS)
    q2, kn, vn, kc, vc = pl.pallas_call(
        qkv_kernel,
        out_shape=(pltpu.VMEM((B * ROWS, HD), F32), pltpu.VMEM((B * 8, HD), F32), pltpu.VMEM((B * 8, HD), F32),
                   pltpu.VMEM(kc.shape, BF16), pltpu.VMEM(vc.shape, BF16)),
        in_specs=[smem(), vmem(), hbm(), hbm(), hbm(), hbm(), hbm()],
        out_specs=(vmem(),) * 5,
        scratch_shapes=[
            pltpu.VMEM((B, D), BF16), pltpu.VMEM((D // HD, HD), BF16),
            pltpu.VMEM((D, QCOLS), BF16), pltpu.VMEM((B, D), BF16), pltpu.VMEM((KVL, GRP + 2, B, HD), F32),
            dma(2), dma(4 * WPARTS + 2 * CPARTS), dma(nch), dma(nch), dma(nch), dma(nch), dma(nch), dma(nch),
        ],
        compiler_params=pltpu.CompilerParams(collective_id=0, has_side_effects=True, vmem_limit_bytes=MIB * 16),
        name="qkv",
    )(in_hbm(ctx_len), in_hbm(freq), in_hbm(x_in), in_hbm(g_attn.reshape(D // HD, HD)), in_hbm(w_qkv), in_hbm(kc), in_hbm(vc))

    part, kc, vc, k_out, v_out = pl.pallas_call(
        attn_kernel,
        out_shape=(pltpu.VMEM((KVL, GRP + 1, B, HD), F32), pltpu.VMEM(kc.shape, BF16), pltpu.VMEM(vc.shape, BF16),
                   jax.ShapeDtypeStruct(kc.shape, BF16), jax.ShapeDtypeStruct(vc.shape, BF16)),
        in_specs=[smem(), vmem(), vmem(), vmem(), vmem(), vmem()],
        out_specs=(vmem(), vmem(), vmem(), hbm(), hbm()),
        scratch_shapes=[
            pltpu.VMEM((2 * ROWS, KVL * T), F32),
            pltpu.VMEM((B * ROWS, HD), F32), pltpu.VMEM((B * ROWS, HD), F32), pltpu.VMEM((B * ROWS, HD), F32),
            dma(2, B // 4),
        ],
        input_output_aliases={4: 1, 5: 2},
        compiler_params=pltpu.CompilerParams(vmem_limit_bytes=MIB * 4),
        name="attn",
    )(in_hbm(ctx_len), q2, kn, vn, kc, vc)

    x_out = pl.pallas_call(
        tail_kernel,
        out_shape=pltpu.VMEM((B, D), BF16),
        in_specs=[vmem(), hbm(), hbm(), hbm(), hbm(), hbm(), hbm()],
        out_specs=vmem(),
        scratch_shapes=[
            pltpu.VMEM((B, D), BF16), pltpu.VMEM((D // HD, HD), BF16), pltpu.VMEM(w_o.shape, BF16), pltpu.VMEM((FFL, D), BF16), pltpu.VMEM((FFL, D), BF16),
            pltpu.VMEM((3, GRP + 1, B, HD), F32), pltpu.VMEM((B, GRP * HD), BF16), pltpu.VMEM((B, D), BF16), pltpu.VMEM((B, FFL), BF16),
            pltpu.VMEM((NCH, 8, B, HD), F32), pltpu.VMEM((NCH, 4, B, HD), F32),
            pltpu.VMEM((NCH, 4, B, HD), F32), pltpu.VMEM((NCH, 4, B, HD), F32),
            pltpu.VMEM((NCH, 3, B, HD), F32), pltpu.VMEM((NCH, 3, B, HD), F32),
            pltpu.VMEM((D // HD, B, HD), F32), pltpu.VMEM((D // HD, B, HD), F32),
            dma(2), pltpu.SemaphoreType.DMA, dma(2, 7), dma(7), dma(3), dma(3),
            dma(2, NCH), dma(2, NCH), dma(2, NCH, 3), dma(2, NCH, 3), dma(2, NCH, 4), dma(2, NCH, 4), dma(2, NCH, 3), dma(2, NCH, 3),
        ],
        compiler_params=pltpu.CompilerParams(collective_id=1, has_side_effects=True, vmem_limit_bytes=TAIL_VMEM),
        cost_estimate=pl.CostEstimate(flops=10 ** 10, bytes_accessed=10 ** 8, transcendentals=0),
        name="tail",
    )(in_vmem(part), in_hbm(x_in), in_hbm(g_mlp.reshape(D // HD, HD)), in_hbm(w_o), in_hbm(w_gate.T), in_hbm(w_up.T), in_hbm(w_down))
    return x_out, k_out.reshape(k_cache.shape), v_out.reshape(v_cache.shape)


def solution(mesh):
    x_spec = P("dp", None)
    cache_spec = P("dp", "kvp", "tp", None)
    model_axes = ("tp", "kvp")
    in_specs = (x_spec, P("dp"), P(None), P(None), P(None, "tp"), P(model_axes, None), P(None, model_axes), P(None, model_axes), P(model_axes, None), cache_spec, cache_spec)
    return jax.shard_map(layer_step, mesh=mesh, in_specs=in_specs, out_specs=(x_spec, cache_spec, cache_spec), check_vma=False)
```

```python
import jax
import jax.numpy as jnp
import numpy as np
from jax import lax
from jax.experimental import pallas as pl
from jax.experimental.pallas import tpu as pltpu
from jax.sharding import PartitionSpec as P

ROPE_THETA = 500000.0
EPS = 1e-5
NEG_FILL = -1e30
MESH = pl.DeviceIdType.MESH
F32 = jnp.float32
BF16 = jnp.bfloat16

D = 5120
HD = 128
B = 32
T = 256
KVL = 4
GRP = 5
ROWS = 24
QCOLS = (GRP + 2) * HD
FFL = 1728
MIB = 1024 * 1024
TAIL_VMEM = 56 * MIB


def remote(src, dst, send, recv, dev):
    return pltpu.make_async_remote_copy(src_ref=src, dst_ref=dst, send_sem=send, recv_sem=recv, device_id=dev, device_id_type=MESH)


def enter(peers):
    barrier = pltpu.get_barrier_semaphore()
    for peer in peers:
        pl.semaphore_signal(barrier, inc=1, device_id=peer, device_id_type=MESH)
    pl.semaphore_wait(barrier, len(peers))


WPARTS = 4
CPARTS = 8
FLIGHT = 6
CHUNKS = ((0, 2), (2, 2), (4, 2), (6, 1))


def qkv_kernel(ctx_ref, freq_ref, x_hbm, g_hbm, w_ref, k_hbm, v_hbm, q_ref, kn_ref, vn_ref, kc_ref, vc_ref,
               x_ref, g_ref, wbuf, u_ref, ex, x_sem, w_sem, m_send, m_recv, x_send, x_recv, r_send, r_recv):
    j = lax.axis_index("kvp")
    mate = {"kvp": j + 1 - 2 * lax.rem(j, 2)}
    side = {"kvp": lax.rem(j + 2, 4)}
    x_copy = pltpu.make_async_copy(x_hbm, x_ref, x_sem.at[0])
    g_copy = pltpu.make_async_copy(g_hbm, g_ref, x_sem.at[1])
    x_copy.start()
    g_copy.start()

    pieces = []
    last_piece = []
    for first, n in CHUNKS:
        depth = D * 2 // (WPARTS * n)
        for part in range(D // depth):
            rows = pl.ds(part * depth, depth)
            cols = pl.ds(pl.multiple_of(j * QCOLS + first * HD, HD), n * HD)
            pieces.append((w_ref.at[rows, cols], wbuf.at[rows, pl.ds(first * HD, n * HD)]))
        last_piece.append(len(pieces))
    n_weight = len(pieces)
    for i in range(2 * CPARTS):
        src, dst = ((k_hbm, kc_ref), (v_hbm, vc_ref))[i // CPARTS]
        some = pl.ds((i % CPARTS) * (B // CPARTS), B // CPARTS)
        pieces.append((src.at[some], dst.at[some, pl.ds(0, KVL * T)]))

    def fetch(i):
        return pltpu.make_async_copy(*pieces[i], w_sem.at[i])

    for i in range(FLIGHT):
        fetch(i).start()
    enter((mate, side))
    row = lax.broadcasted_iota(jnp.int32, (B, HD), 0)
    lane = lax.broadcasted_iota(jnp.int32, (B, HD), 1)
    ctx = jnp.zeros((B, HD), F32)
    for b in range(B):
        ctx = jnp.where(row == b, ctx_ref[b].astype(F32), ctx)
    angles = ctx * freq_ref[...]
    cos_t = jnp.cos(angles)
    sin_t = jnp.sin(angles)
    sin_t = jnp.where(lane < HD // 2, -sin_t, sin_t)
    x_copy.wait()
    g_copy.wait()
    squares = jnp.zeros((B, HD), F32)
    for i in range(D // HD):
        xf = x_ref[:, i * HD:(i + 1) * HD].astype(F32)
        squares = squares + xf * xf
    inv = lax.rsqrt(jnp.sum(squares, axis=-1, keepdims=True) / D + EPS)
    for i in range(D // HD):
        xf = x_ref[:, i * HD:(i + 1) * HD].astype(F32)
        u_ref[:, i * HD:(i + 1) * HD] = (xf * inv * g_ref[i:i + 1, :].astype(F32)).astype(BF16)
    q_ref[...] = jnp.zeros_like(q_ref)

    def piece(slot, i):
        first, n = CHUNKS[i]
        return ex.at[slot, pl.ds(first, n)]

    def to_mate(i):
        return remote(piece(j, i), piece(j, i), m_send.at[i], m_recv.at[i], mate)

    def to_side(i):
        return remote(piece(j, i), piece(j, i), x_send.at[i], x_recv.at[i], side)

    def relay(i):
        slot = lax.rem(j + 2, 4)
        return remote(piece(slot, i), piece(slot, i), r_send.at[i], r_recv.at[i], mate)

    for i, (first, n) in enumerate(CHUNKS):
        for p in range(last_piece[i - 1] if i else 0, last_piece[i]):
            fetch(p).wait()
            fetch(p + FLIGHT).start()
        if i == len(CHUNKS) - 1:
            for p in range(n_weight + FLIGHT, len(pieces)):
                fetch(p).start()
        res = jnp.dot(u_ref[...], wbuf[:, first * HD:(first + n) * HD], preferred_element_type=F32)
        for h in range(n):
            tile = res[:, h * HD:(h + 1) * HD]
            if first + h < GRP + 1:
                tile = tile * cos_t + pltpu.roll(tile, HD // 2, 1) * sin_t
            ex[j, first + h] = tile
        to_side(i).start()
        to_mate(i).start()
    for i in range(len(CHUNKS)):
        to_side(i).wait_recv()
        relay(i).start()
    for i in range(len(CHUNKS)):
        to_mate(i).wait_recv()
        relay(i).wait_recv()
    for g in range(KVL):
        for r in range(GRP):
            q_ref[pl.ds(g * GRP + r, B, stride=ROWS), :] = ex[g, r]
        kn = ex[g, GRP]
        vn = ex[g, GRP + 1]
        for half in range(2):
            kn_ref[pl.ds(half * KVL + g, B, stride=8), :] = kn
            vn_ref[pl.ds(half * KVL + g, B, stride=8), :] = vn
    for i in range(len(CHUNKS)):
        to_side(i).wait_send()
        to_mate(i).wait_send()
        relay(i).wait_send()
    for i in range(n_weight, len(pieces)):
        fetch(i).wait()


PAIRS = B // 2
CPITCH = KVL * T + 16


def attn_kernel(ctx_ref, q_ref, kn_ref, vn_ref, k_ref, v_ref, part_ref, kbuf, vbuf, ko_ref, vo_ref, bias, acc2, m2, l2, out_sem):
    base = lax.axis_index("kvp") * T

    def flush(i, which):
        src, dst = ((kbuf, ko_ref), (vbuf, vo_ref))[which]
        some = pl.ds(4 * i, 4)
        return pltpu.make_async_copy(src.at[some, pl.ds(0, KVL * T)], dst.at[some], out_sem.at[which, i])

    row = lax.broadcasted_iota(jnp.int32, (2 * ROWS, KVL * T), 0)
    row = jnp.where(row >= ROWS, row - ROWS, row)
    col = lax.broadcasted_iota(jnp.int32, (2 * ROWS, KVL * T), 1)
    head = (row >= GRP).astype(jnp.int32) + (row >= 2 * GRP).astype(jnp.int32) + (row >= 3 * GRP).astype(jnp.int32)
    bias[...] = jnp.where(head == (col & (KVL - 1)), 0.0, NEG_FILL)
    first_half = lax.broadcasted_iota(jnp.int32, (2 * ROWS, 1), 0) < ROWS
    wrow = lax.broadcasted_iota(jnp.int32, (16, HD), 0)

    def patch(b):
        pos = ctx_ref[b] - base
        here = (pos >= 0) & (pos < T)
        pos = jnp.clip(pos, 0, T - 1)
        win = pl.ds(pl.multiple_of((pos // 4) * 16, 16), 16)
        hit = (wrow // KVL) == jnp.where(here, pos & 3, 4)
        for new_ref, buf in ((kn_ref, kbuf), (vn_ref, vbuf)):
            new8 = new_ref[pl.ds(b * 8, 8), :]
            new16 = jnp.concatenate([new8, new8], axis=0)
            buf[b, win, :] = jnp.where(hit, new16, buf[b, win, :].astype(F32)).astype(BF16)

    def attend(p):
        b = 2 * p
        q = q_ref[pl.ds(p * 2 * ROWS, 2 * ROWS), :]
        lhs = jnp.concatenate([jnp.where(first_half, q, 0.0), jnp.where(first_half, 0.0, q)], axis=1).astype(BF16)
        keys = jnp.concatenate([kbuf[b, :KVL * T], kbuf[b + 1, :KVL * T]], axis=1)
        s = lax.dot_general(lhs, keys, (((1,), (1,)), ((), ())), preferred_element_type=F32)
        lim = jnp.where(first_half, (ctx_ref[b] - base + 1) * KVL, (ctx_ref[b + 1] - base + 1) * KVL)
        cols = lax.broadcasted_iota(jnp.int32, (2 * ROWS, KVL * T), 1)
        s = jnp.where(cols < lim, s * HD ** -0.5 + bias[...], NEG_FILL)
        m = jnp.max(s, axis=1, keepdims=True)
        w = jnp.exp(s - m)
        values = jnp.concatenate([vbuf[b, :KVL * T], vbuf[b + 1, :KVL * T]], axis=1)
        o = jnp.dot(w.astype(BF16), values, preferred_element_type=F32)
        rows = pl.ds(p * 2 * ROWS, 2 * ROWS)
        acc2[rows, :] = jnp.where(first_half, o[:, :HD], o[:, HD:])
        m2[rows, :] = jnp.broadcast_to(m, (2 * ROWS, HD))
        l2[rows, :] = jnp.broadcast_to(jnp.sum(w, axis=1, keepdims=True), (2 * ROWS, HD))

    @pl.loop(0, B // 4)
    def _(it):
        for k in range(4):
            patch(it * 4 + k)
        flush(it, 0).start()
        flush(it, 1).start()

    @pl.loop(0, PAIRS // 4)
    def _(it):
        for k in range(4):
            attend(it * 4 + k)

    lane = lax.broadcasted_iota(jnp.int32, (B, HD), 1)
    for g in range(KVL):
        stats = jnp.zeros((B, HD), F32)
        for r in range(GRP):
            rows = pl.ds(g * GRP + r, B, stride=ROWS)
            part_ref[g, r] = acc2[rows, :]
            stats = jnp.where(lane == r, m2[rows, :], stats)
            stats = jnp.where(lane == 8 + r, l2[rows, :], stats)
        part_ref[g, GRP] = stats

    @pl.loop(0, B // 4)
    def _(i):
        flush(i, 0).wait()
        flush(i, 1).wait()


NCH = 5
CW = D // NCH
GCH = 256
FLIP = 4
AHEAD = 3
FLIPS = (4, 1, 3, 3, 1)


def tail_kernel(part_ref, x_hbm, g_hbm, wo_hbm, wg_hbm, wu_hbm, wd_hbm, out_ref,
                x_ref, g_ref, wo, w2, rx, attn, n_ref, y_ref, pbuf, sbuf, pair_a, pair_b, rs_a, rs_b, ag_a, ag_b,
                x_sem, w_sem, gu_sem, wd_sem, c_send, c_recv, d_send, d_recv, s_send, s_recv, a_send, a_recv, f_send, f_recv):
    t = lax.axis_index("tp")
    j = lax.axis_index("kvp")
    core = lax.rem(j, 2)
    xpos = j // 2
    quarter = t * 2 + xpos
    mate = {"tp": t, "kvp": j + 1 - 2 * core}
    chips = []
    for e in (1, 2, 3):
        tt = t if e == 1 else 1 - t
        xx = xpos if e == 2 else 1 - xpos
        chips.append(({"tp": tt, "kvp": xx * 2 + core}, tt * 2 + xx))
    ring = [{"tp": t, "kvp": lax.rem(j + d, 4)} for d in (1, 2, 3)]

    full = FFL // GCH
    rest = FFL - full * GCH
    spans = [(i * GCH, GCH) for i in range(full)] + [(full * GCH, rest)]

    def gate_copy(i, which):
        first, n = spans[i]
        src = (wg_hbm, wu_hbm)[which]
        return pltpu.make_async_copy(src.at[pl.ds(first, n)], w2.at[which, pl.ds(first, n), pl.ds(0, D)], gu_sem.at[which, i])

    order = [(i, which) for i in range(len(spans)) for which in range(2)]
    for block in range(AHEAD - 1):
        gate_copy(*order[block]).start()
    wo_copy = pltpu.make_async_copy(wo_hbm, wo, w_sem)
    wo_copy.start()
    gate_copy(*order[AHEAD - 1]).start()
    x_copy = pltpu.make_async_copy(x_hbm, x_ref, x_sem.at[0])
    g_copy = pltpu.make_async_copy(g_hbm, g_ref, x_sem.at[1])
    x_copy.start()
    g_copy.start()
    enter(tuple(ring) + (chips[1][0], chips[2][0]))

    def combine_copy(d):
        return remote(part_ref.at[lax.rem(j + d, 4)], rx.at[d - 1], c_send.at[d - 1], c_recv.at[d - 1], ring[d - 1])

    for d in (2, 1, 3):
        combine_copy(d).start()

    def down_copy(i):
        rows = pl.ds(*spans[i])
        return pltpu.make_async_copy(wd_hbm.at[rows], w2.at[0, rows, pl.ds(0, D)], wd_sem.at[i])


    flipped = [0]

    def flip(blocks):
        for block in range(flipped[0], flipped[0] + blocks):
            i, which = order[block]
            gate_copy(i, which).wait()
            if block + AHEAD < len(order):
                gate_copy(*order[block + AHEAD]).start()

            @pl.loop(0, D // (GCH * FLIP))
            def _(u):
                for v in range(FLIP):
                    rows = pl.ds(i * GCH, GCH)
                    cols = pl.ds(pl.multiple_of((u * FLIP + v) * GCH, GCH), GCH)
                    w2[which, rows, cols] = w2[which, rows, cols].T
        flipped[0] += blocks

    flip(FLIPS[0])
    wo_copy.wait()
    x_copy.wait()
    g_copy.wait()
    for d in (1, 2, 3):
        combine_copy(d).wait_recv()
    stats = [part_ref[j, GRP]] + [rx[i, GRP] for i in range(3)]
    for r in range(GRP):
        ms = [s[:, r:r + 1] for s in stats]
        top = jnp.maximum(jnp.maximum(ms[0], ms[1]), jnp.maximum(ms[2], ms[3]))
        scales = [jnp.exp(m - top) for m in ms]
        denom = sum(sc * s[:, 8 + r:9 + r] for sc, s in zip(scales, stats))
        total = part_ref[j, r] * scales[0]
        for i in range(3):
            total = total + rx[i, r] * scales[i + 1]
        attn[:, r * HD:(r + 1) * HD] = (total / denom).astype(BF16)

    def all_sum(which, product, base, pair, rs, ag):
        def pair_copy(k):
            return remote(pbuf.at[k, pl.ds((1 - core) * 4, 4)], pair.at[k], d_send.at[which, k], d_recv.at[which, k], mate)

        def scatter_copy(k, e):
            dev, q = chips[e]
            return remote(sbuf.at[k, q], rs.at[k, e], s_send.at[which, k, e], s_recv.at[which, k, e], dev)

        own = core * 4 + quarter

        def gather_copy(k, e):
            dev = mate if e == 3 else chips[e][0]
            return remote(ag.at[k * 8 + own], ag.at[k * 8 + own], a_send.at[which, k, e], a_recv.at[which, k, e], dev)

        def forward_copy(k, e):
            slot = k * 8 + core * 4 + chips[e][1]
            return remote(ag.at[slot], ag.at[slot], f_send.at[which, k, e], f_recv.at[which, k, e], mate)

        for k in range(NCH):
            res = product(k)
            for i in range(8):
                pbuf[k, i] = res[:, i * HD:(i + 1) * HD]
            pair_copy(k).start()
        if which == 0:
            flip(FLIPS[1])
        for k in range(NCH):
            pair_copy(k).wait_recv()
            for i in range(4):
                sbuf[k, i] = pbuf[k, core * 4 + i] + pair[k, i]
            for e in (2, 0, 1):
                scatter_copy(k, e).start()
        if which == 0:
            flip(FLIPS[2])
        for k in range(NCH):
            for e in range(3):
                scatter_copy(k, e).wait_recv()
            total = sbuf[k, quarter] + rs[k, 0] + rs[k, 1] + rs[k, 2]
            ag[k * 8 + own] = (base(k * 8 + own) + total).astype(BF16).astype(F32)
            for e in (2, 0, 1, 3):
                gather_copy(k, e).start()
        if which == 0:
            flip(FLIPS[3])
        for k in range(NCH):
            for e in range(3):
                gather_copy(k, e).wait_recv()
                forward_copy(k, e).start()
        if which == 0:
            flip(FLIPS[4])
            for block in range(sum(FLIPS) + AHEAD, len(order)):
                gate_copy(*order[block]).start()
        for k in range(NCH):
            gather_copy(k, 3).wait_recv()
            for e in range(3):
                forward_copy(k, e).wait_recv()
        for k in range(NCH):
            pair_copy(k).wait_send()
            for e in range(3):
                scatter_copy(k, e).wait_send()
                forward_copy(k, e).wait_send()
            for e in range(4):
                gather_copy(k, e).wait_send()

    def o_product(k):
        return jnp.dot(attn[...], wo[:, k * CW:(k + 1) * CW], preferred_element_type=F32)

    def x_base(i):
        return x_ref[:, pl.ds(pl.multiple_of(i * HD, HD), HD)].astype(F32)

    all_sum(0, o_product, x_base, pair_a, rs_a, ag_a)

    squares = jnp.zeros((B, HD), F32)
    for i in range(D // HD):
        squares = squares + ag_a[i] * ag_a[i]
    inv = lax.rsqrt(jnp.sum(squares, axis=-1, keepdims=True) / D + EPS)
    for i in range(D // HD):
        n_ref[:, i * HD:(i + 1) * HD] = (ag_a[i] * inv * g_ref[i:i + 1, :].astype(F32)).astype(BF16)

    def act(gate, up):
        return (jax.nn.silu(gate) * up).astype(BF16)

    for i, (first, n) in enumerate(spans):
        rows = pl.ds(first, n)
        for which in range(2):
            if 2 * i + which >= sum(FLIPS):
                gate_copy(i, which).wait()
        sums = [None, None]
        for k in range(D // GCH):
            cols = slice(k * GCH, (k + 1) * GCH)
            for which in range(2):
                dims = (((1,), (0 if 2 * i + which < sum(FLIPS) else 1,)), ((), ()))
                term = lax.dot_general(n_ref[:, cols], w2[which, rows, cols], dims, preferred_element_type=F32)
                sums[which] = term if k == 0 else sums[which] + term
        y_ref[:, first:first + n] = act(sums[0], sums[1])
        down_copy(i).start()
    for i in range(len(spans)):
        down_copy(i).wait()

    def down_product(k):
        return jnp.dot(y_ref[...], w2[0, :, k * CW:(k + 1) * CW], preferred_element_type=F32)

    all_sum(1, down_product, lambda i: ag_a[i], pair_b, rs_b, ag_b)
    for i in range(D // HD):
        out_ref[:, i * HD:(i + 1) * HD] = ag_b[i].astype(BF16)
    for d in (1, 2, 3):
        combine_copy(d).wait_send()


def vmem():
    return pl.BlockSpec(memory_space=pltpu.VMEM)


def hbm():
    return pl.BlockSpec(memory_space=pl.ANY)


def in_hbm(a):
    return pltpu.with_memory_space_constraint(a, pltpu.HBM)


def in_vmem(a):
    return pltpu.with_memory_space_constraint(a, pltpu.VMEM)


def smem():
    return pl.BlockSpec(memory_space=pltpu.SMEM)


def dma(*shape):
    return pltpu.SemaphoreType.DMA(shape)


def layer_step(x_in, ctx_len, g_attn, g_mlp, w_qkv, w_o, w_gate, w_up, w_down, k_cache, v_cache):
    freq = ROPE_THETA ** (-2.0 * np.arange(HD // 2, dtype=np.float64) / HD)
    freq = np.concatenate([freq, freq]).astype(np.float32).reshape(1, HD)
    kc = k_cache.reshape(B, T * KVL, HD)
    vc = v_cache.reshape(B, T * KVL, HD)
    nch = len(CHUNKS)
    q2, kn, vn, kv, vv = pl.pallas_call(
        qkv_kernel,
        out_shape=(pltpu.VMEM((B * ROWS, HD), F32), pltpu.VMEM((B * 8, HD), F32), pltpu.VMEM((B * 8, HD), F32),
                   pltpu.VMEM((B, CPITCH, HD), BF16), pltpu.VMEM((B, CPITCH, HD), BF16)),
        in_specs=[smem(), vmem(), hbm(), hbm(), hbm(), hbm(), hbm()],
        out_specs=(vmem(),) * 5,
        scratch_shapes=[
            pltpu.VMEM((B, D), BF16), pltpu.VMEM((D // HD, HD), BF16),
            pltpu.VMEM((D, QCOLS), BF16), pltpu.VMEM((B, D), BF16), pltpu.VMEM((KVL, GRP + 2, B, HD), F32),
            dma(2), dma(4 * WPARTS + 2 * CPARTS), dma(nch), dma(nch), dma(nch), dma(nch), dma(nch), dma(nch),
        ],
        compiler_params=pltpu.CompilerParams(collective_id=0, has_side_effects=True, vmem_limit_bytes=MIB * 16),
        name="qkv",
    )(in_hbm(ctx_len), in_hbm(freq), in_hbm(x_in), in_hbm(g_attn.reshape(D // HD, HD)), in_hbm(w_qkv), in_hbm(kc), in_hbm(vc))

    part, _, _, k_out, v_out = pl.pallas_call(
        attn_kernel,
        out_shape=(pltpu.VMEM((KVL, GRP + 1, B, HD), F32), pltpu.VMEM((B, CPITCH, HD), BF16), pltpu.VMEM((B, CPITCH, HD), BF16),
                   jax.ShapeDtypeStruct(kc.shape, BF16), jax.ShapeDtypeStruct(vc.shape, BF16)),
        in_specs=[smem(), vmem(), vmem(), vmem(), vmem(), vmem()],
        out_specs=(vmem(), vmem(), vmem(), hbm(), hbm()),
        scratch_shapes=[
            pltpu.VMEM((2 * ROWS, KVL * T), F32),
            pltpu.VMEM((B * ROWS, HD), F32), pltpu.VMEM((B * ROWS, HD), F32), pltpu.VMEM((B * ROWS, HD), F32),
            dma(2, B // 4),
        ],
        input_output_aliases={4: 1, 5: 2},
        compiler_params=pltpu.CompilerParams(vmem_limit_bytes=MIB * 4),
        name="attn",
    )(in_hbm(ctx_len), q2, kn, vn, kv, vv)

    x_out = pl.pallas_call(
        tail_kernel,
        out_shape=pltpu.VMEM((B, D), BF16),
        in_specs=[vmem(), hbm(), hbm(), hbm(), hbm(), hbm(), hbm()],
        out_specs=vmem(),
        scratch_shapes=[
            pltpu.VMEM((B, D), BF16), pltpu.VMEM((D // HD, HD), BF16), pltpu.VMEM(w_o.shape, BF16), pltpu.VMEM((2, FFL, D + HD), BF16),
            pltpu.VMEM((3, GRP + 1, B, HD), F32), pltpu.VMEM((B, GRP * HD), BF16), pltpu.VMEM((B, D), BF16), pltpu.VMEM((B, FFL), BF16),
            pltpu.VMEM((NCH, 8, B, HD), F32), pltpu.VMEM((NCH, 4, B, HD), F32),
            pltpu.VMEM((NCH, 4, B, HD), F32), pltpu.VMEM((NCH, 4, B, HD), F32),
            pltpu.VMEM((NCH, 3, B, HD), F32), pltpu.VMEM((NCH, 3, B, HD), F32),
            pltpu.VMEM((D // HD, B, HD), F32), pltpu.VMEM((D // HD, B, HD), F32),
            dma(2), pltpu.SemaphoreType.DMA, dma(2, 7), dma(7), dma(3), dma(3),
            dma(2, NCH), dma(2, NCH), dma(2, NCH, 3), dma(2, NCH, 3), dma(2, NCH, 4), dma(2, NCH, 4), dma(2, NCH, 3), dma(2, NCH, 3),
        ],
        compiler_params=pltpu.CompilerParams(collective_id=1, has_side_effects=True, vmem_limit_bytes=TAIL_VMEM),
        cost_estimate=pl.CostEstimate(flops=10 ** 10, bytes_accessed=10 ** 8, transcendentals=0),
        name="tail",
    )(in_vmem(part), in_hbm(x_in), in_hbm(g_mlp.reshape(D // HD, HD)), in_hbm(w_o), in_hbm(w_gate.T), in_hbm(w_up.T), in_hbm(w_down))
    return x_out, k_out.reshape(k_cache.shape), v_out.reshape(v_cache.shape)


def solution(mesh):
    x_spec = P("dp", None)
    cache_spec = P("dp", "kvp", "tp", None)
    model_axes = ("tp", "kvp")
    in_specs = (x_spec, P("dp"), P(None), P(None), P(None, "tp"), P(model_axes, None), P(None, model_axes), P(None, model_axes), P(model_axes, None), cache_spec, cache_spec)
    return jax.shard_map(layer_step, mesh=mesh, in_specs=in_specs, out_specs=(x_spec, cache_spec, cache_spec), check_vma=False)
```

```python
import jax
import jax.numpy as jnp
import numpy as np
from jax import lax
from jax.experimental import pallas as pl
from jax.experimental.pallas import tpu as pltpu
from jax.sharding import PartitionSpec as P

ROPE_THETA = 500000.0
EPS = 1e-5
NEG_FILL = -1e30
MESH = pl.DeviceIdType.MESH
F32 = jnp.float32
BF16 = jnp.bfloat16

D = 5120
HD = 128
B = 32
T = 256
KVL = 4
GRP = 5
ROWS = 24
QCOLS = (GRP + 2) * HD
FFL = 1728
MIB = 1024 * 1024
TAIL_VMEM = 56 * MIB


def remote(src, dst, send, recv, dev):
    return pltpu.make_async_remote_copy(src_ref=src, dst_ref=dst, send_sem=send, recv_sem=recv, device_id=dev, device_id_type=MESH)


def enter(peers):
    barrier = pltpu.get_barrier_semaphore()
    for peer in peers:
        pl.semaphore_signal(barrier, inc=1, device_id=peer, device_id_type=MESH)
    pl.semaphore_wait(barrier, len(peers))


WPARTS = 4
CPARTS = 8
FLIGHT = 6
CHUNKS = ((0, 2), (2, 2), (4, 2), (6, 1))


def qkv_kernel(ctx_ref, freq_ref, x_hbm, g_hbm, w_ref, k_hbm, v_hbm, q_ref, kn_ref, vn_ref, kc_ref, vc_ref,
               x_ref, g_ref, wbuf, u_ref, ex, x_sem, w_sem, m_send, m_recv, x_send, x_recv, r_send, r_recv):
    j = lax.axis_index("kvp")
    mate = {"kvp": j + 1 - 2 * lax.rem(j, 2)}
    side = {"kvp": lax.rem(j + 2, 4)}
    x_copy = pltpu.make_async_copy(x_hbm, x_ref, x_sem.at[0])
    g_copy = pltpu.make_async_copy(g_hbm, g_ref, x_sem.at[1])
    x_copy.start()
    g_copy.start()

    pieces = []
    last_piece = []
    for first, n in CHUNKS:
        depth = D * 2 // (WPARTS * n)
        for part in range(D // depth):
            rows = pl.ds(part * depth, depth)
            cols = pl.ds(pl.multiple_of(j * QCOLS + first * HD, HD), n * HD)
            pieces.append((w_ref.at[rows, cols], wbuf.at[rows, pl.ds(first * HD, n * HD)]))
        last_piece.append(len(pieces))
    n_weight = len(pieces)
    for i in range(2 * CPARTS):
        src, dst = ((k_hbm, kc_ref), (v_hbm, vc_ref))[i // CPARTS]
        some = pl.ds((i % CPARTS) * (B // CPARTS), B // CPARTS)
        pieces.append((src.at[some], dst.at[some, pl.ds(0, KVL * T)]))

    def fetch(i):
        return pltpu.make_async_copy(*pieces[i], w_sem.at[i])

    for i in range(FLIGHT):
        fetch(i).start()
    enter((mate, side))
    row = lax.broadcasted_iota(jnp.int32, (B, HD), 0)
    lane = lax.broadcasted_iota(jnp.int32, (B, HD), 1)
    ctx = jnp.zeros((B, HD), F32)
    for b in range(B):
        ctx = jnp.where(row == b, ctx_ref[b].astype(F32), ctx)
    angles = ctx * freq_ref[...]
    cos_t = jnp.cos(angles)
    sin_t = jnp.sin(angles)
    sin_t = jnp.where(lane < HD // 2, -sin_t, sin_t)
    x_copy.wait()
    g_copy.wait()
    squares = jnp.zeros((B, HD), F32)
    for i in range(D // HD):
        xf = x_ref[:, i * HD:(i + 1) * HD].astype(F32)
        squares = squares + xf * xf
    inv = lax.rsqrt(jnp.sum(squares, axis=-1, keepdims=True) / D + EPS)
    for i in range(D // HD):
        xf = x_ref[:, i * HD:(i + 1) * HD].astype(F32)
        u_ref[:, i * HD:(i + 1) * HD] = (xf * inv * g_ref[i:i + 1, :].astype(F32)).astype(BF16)
    q_ref[...] = jnp.zeros_like(q_ref)

    def piece(slot, i):
        first, n = CHUNKS[i]
        return ex.at[slot, pl.ds(first, n)]

    def to_mate(i):
        return remote(piece(j, i), piece(j, i), m_send.at[i], m_recv.at[i], mate)

    def to_side(i):
        return remote(piece(j, i), piece(j, i), x_send.at[i], x_recv.at[i], side)

    def relay(i):
        slot = lax.rem(j + 2, 4)
        return remote(piece(slot, i), piece(slot, i), r_send.at[i], r_recv.at[i], mate)

    for i, (first, n) in enumerate(CHUNKS):
        for p in range(last_piece[i - 1] if i else 0, last_piece[i]):
            fetch(p).wait()
            fetch(p + FLIGHT).start()
        if i == len(CHUNKS) - 1:
            for p in range(n_weight + FLIGHT, len(pieces)):
                fetch(p).start()
        res = jnp.dot(u_ref[...], wbuf[:, first * HD:(first + n) * HD], preferred_element_type=F32)
        for h in range(n):
            tile = res[:, h * HD:(h + 1) * HD]
            if first + h < GRP + 1:
                tile = tile * cos_t + pltpu.roll(tile, HD // 2, 1) * sin_t
            ex[j, first + h] = tile
        to_side(i).start()
        to_mate(i).start()
    for i in range(len(CHUNKS)):
        to_side(i).wait_recv()
        relay(i).start()
    for i in range(len(CHUNKS)):
        to_mate(i).wait_recv()
        relay(i).wait_recv()
    for g in range(KVL):
        for r in range(GRP):
            q_ref[pl.ds(g * GRP + r, B, stride=ROWS), :] = ex[g, r]
        kn = ex[g, GRP]
        vn = ex[g, GRP + 1]
        for half in range(2):
            kn_ref[pl.ds(half * KVL + g, B, stride=8), :] = kn
            vn_ref[pl.ds(half * KVL + g, B, stride=8), :] = vn
    for i in range(len(CHUNKS)):
        to_side(i).wait_send()
        to_mate(i).wait_send()
        relay(i).wait_send()
    for i in range(n_weight, len(pieces)):
        fetch(i).wait()


PAIRS = B // 2
CPITCH = KVL * T + 16


def attn_kernel(ctx_ref, q_ref, kn_ref, vn_ref, k_ref, v_ref, part_ref, kbuf, vbuf, ko_ref, vo_ref, bias, acc2, m2, l2, out_sem):
    base = lax.axis_index("kvp") * T

    def flush(i, which):
        src, dst = ((kbuf, ko_ref), (vbuf, vo_ref))[which]
        some = pl.ds(4 * i, 4)
        return pltpu.make_async_copy(src.at[some, pl.ds(0, KVL * T)], dst.at[some], out_sem.at[which, i])

    row = lax.broadcasted_iota(jnp.int32, (2 * ROWS, KVL * T), 0)
    row = jnp.where(row >= ROWS, row - ROWS, row)
    col = lax.broadcasted_iota(jnp.int32, (2 * ROWS, KVL * T), 1)
    head = (row >= GRP).astype(jnp.int32) + (row >= 2 * GRP).astype(jnp.int32) + (row >= 3 * GRP).astype(jnp.int32)
    bias[...] = jnp.where(head == (col & (KVL - 1)), 0.0, NEG_FILL)
    first_half = lax.broadcasted_iota(jnp.int32, (2 * ROWS, 1), 0) < ROWS
    wrow = lax.broadcasted_iota(jnp.int32, (16, HD), 0)

    def patch(b):
        pos = ctx_ref[b] - base
        here = (pos >= 0) & (pos < T)
        pos = jnp.clip(pos, 0, T - 1)
        win = pl.ds(pl.multiple_of((pos // 4) * 16, 16), 16)
        hit = (wrow // KVL) == jnp.where(here, pos & 3, 4)
        for new_ref, buf in ((kn_ref, kbuf), (vn_ref, vbuf)):
            new8 = new_ref[pl.ds(b * 8, 8), :]
            new16 = jnp.concatenate([new8, new8], axis=0)
            buf[b, win, :] = jnp.where(hit, new16, buf[b, win, :].astype(F32)).astype(BF16)

    def attend(p):
        b = 2 * p
        q = q_ref[pl.ds(p * 2 * ROWS, 2 * ROWS), :]
        lhs = jnp.concatenate([jnp.where(first_half, q, 0.0), jnp.where(first_half, 0.0, q)], axis=1).astype(BF16)
        keys = jnp.concatenate([kbuf[b, :KVL * T], kbuf[b + 1, :KVL * T]], axis=1)
        s = lax.dot_general(lhs, keys, (((1,), (1,)), ((), ())), preferred_element_type=F32)
        lim = jnp.where(first_half, (ctx_ref[b] - base + 1) * KVL, (ctx_ref[b + 1] - base + 1) * KVL)
        cols = lax.broadcasted_iota(jnp.int32, (2 * ROWS, KVL * T), 1)
        s = jnp.where(cols < lim, s * HD ** -0.5 + bias[...], NEG_FILL)
        m = jnp.max(s, axis=1, keepdims=True)
        w = jnp.exp(s - m)
        values = jnp.concatenate([vbuf[b, :KVL * T], vbuf[b + 1, :KVL * T]], axis=1)
        o = jnp.dot(w.astype(BF16), values, preferred_element_type=F32)
        rows = pl.ds(p * 2 * ROWS, 2 * ROWS)
        acc2[rows, :] = jnp.where(first_half, o[:, :HD], o[:, HD:])
        m2[rows, :] = jnp.broadcast_to(m, (2 * ROWS, HD))
        l2[rows, :] = jnp.broadcast_to(jnp.sum(w, axis=1, keepdims=True), (2 * ROWS, HD))

    @pl.loop(0, B // 4)
    def _(it):
        for k in range(4):
            patch(it * 4 + k)
        flush(it, 0).start()
        flush(it, 1).start()

    @pl.loop(0, PAIRS // 4)
    def _(it):
        for k in range(4):
            attend(it * 4 + k)

    lane = lax.broadcasted_iota(jnp.int32, (B, HD), 1)
    for g in range(KVL):
        stats = jnp.zeros((B, HD), F32)
        for r in range(GRP):
            rows = pl.ds(g * GRP + r, B, stride=ROWS)
            part_ref[g, r] = acc2[rows, :]
            stats = jnp.where(lane == r, m2[rows, :], stats)
            stats = jnp.where(lane == 8 + r, l2[rows, :], stats)
        part_ref[g, GRP] = stats

    @pl.loop(0, B // 4)
    def _(i):
        flush(i, 0).wait()
        flush(i, 1).wait()


NCH = 5
CW = D // NCH
GCH = 256
FLIP = 4
AHEAD = 3
FLIPS = (2, 0, 2, 2, 0)


def tail_kernel(part_ref, x_hbm, g_hbm, wo_hbm, wg_hbm, wu_hbm, wd_hbm, out_ref,
                x_ref, g_ref, wo, w2, rx, attn, n_ref, y_ref, pbuf, sbuf, pair_a, pair_b, rs_a, rs_b, ag_a, ag_b,
                x_sem, w_sem, gu_sem, wd_sem, c_send, c_recv, d_send, d_recv, s_send, s_recv, a_send, a_recv, f_send, f_recv):
    t = lax.axis_index("tp")
    j = lax.axis_index("kvp")
    core = lax.rem(j, 2)
    xpos = j // 2
    quarter = t * 2 + xpos
    mate = {"tp": t, "kvp": j + 1 - 2 * core}
    chips = []
    for e in (1, 2, 3):
        tt = t if e == 1 else 1 - t
        xx = xpos if e == 2 else 1 - xpos
        chips.append(({"tp": tt, "kvp": xx * 2 + core}, tt * 2 + xx))
    ring = [{"tp": t, "kvp": lax.rem(j + d, 4)} for d in (1, 2, 3)]

    full = FFL // GCH
    rest = FFL - full * GCH
    spans = [(i * GCH, GCH) for i in range(full)] + [(full * GCH, rest)]

    def gate_copy(i, which):
        first, n = spans[i]
        src = (wg_hbm, wu_hbm)[which]
        return pltpu.make_async_copy(src.at[pl.ds(first, n)], w2.at[which, pl.ds(first, n), pl.ds(0, D)], gu_sem.at[which, i])

    order = [(i, which) for i in range(len(spans)) for which in range(2)]
    for block in range(AHEAD - 1):
        gate_copy(*order[block]).start()
    wo_copy = pltpu.make_async_copy(wo_hbm, wo, w_sem)
    wo_copy.start()
    gate_copy(*order[AHEAD - 1]).start()
    x_copy = pltpu.make_async_copy(x_hbm, x_ref, x_sem.at[0])
    g_copy = pltpu.make_async_copy(g_hbm, g_ref, x_sem.at[1])
    x_copy.start()
    g_copy.start()
    enter(tuple(ring) + (chips[1][0], chips[2][0]))

    def combine_copy(d):
        return remote(part_ref.at[lax.rem(j + d, 4)], rx.at[d - 1], c_send.at[d - 1], c_recv.at[d - 1], ring[d - 1])

    for d in (2, 1, 3):
        combine_copy(d).start()

    def down_copy(i):
        rows = pl.ds(*spans[i])
        return pltpu.make_async_copy(wd_hbm.at[rows], w2.at[0, rows, pl.ds(0, D)], wd_sem.at[i])


    flipped = [0]

    def flip(blocks):
        for block in range(flipped[0], flipped[0] + blocks):
            i, which = order[block]
            gate_copy(i, which).wait()
            if block + AHEAD < len(order):
                gate_copy(*order[block + AHEAD]).start()

            @pl.loop(0, D // (GCH * FLIP))
            def _(u):
                for v in range(FLIP):
                    rows = pl.ds(i * GCH, GCH)
                    cols = pl.ds(pl.multiple_of((u * FLIP + v) * GCH, GCH), GCH)
                    w2[which, rows, cols] = w2[which, rows, cols].T
        flipped[0] += blocks

    flip(FLIPS[0])
    wo_copy.wait()
    x_copy.wait()
    g_copy.wait()
    for d in (1, 2, 3):
        combine_copy(d).wait_recv()
    stats = [part_ref[j, GRP]] + [rx[i, GRP] for i in range(3)]
    for r in range(GRP):
        ms = [s[:, r:r + 1] for s in stats]
        top = jnp.maximum(jnp.maximum(ms[0], ms[1]), jnp.maximum(ms[2], ms[3]))
        scales = [jnp.exp(m - top) for m in ms]
        denom = sum(sc * s[:, 8 + r:9 + r] for sc, s in zip(scales, stats))
        total = part_ref[j, r] * scales[0]
        for i in range(3):
            total = total + rx[i, r] * scales[i + 1]
        attn[:, r * HD:(r + 1) * HD] = (total / denom).astype(BF16)

    def all_sum(which, product, base, pair, rs, ag):
        def pair_copy(k):
            return remote(pbuf.at[k, pl.ds((1 - core) * 4, 4)], pair.at[k], d_send.at[which, k], d_recv.at[which, k], mate)

        def scatter_copy(k, e):
            dev, q = chips[e]
            return remote(sbuf.at[k, q], rs.at[k, e], s_send.at[which, k, e], s_recv.at[which, k, e], dev)

        own = core * 4 + quarter

        def gather_copy(k, e):
            dev = mate if e == 3 else chips[e][0]
            return remote(ag.at[k * 8 + own], ag.at[k * 8 + own], a_send.at[which, k, e], a_recv.at[which, k, e], dev)

        def forward_copy(k, e):
            slot = k * 8 + core * 4 + chips[e][1]
            return remote(ag.at[slot], ag.at[slot], f_send.at[which, k, e], f_recv.at[which, k, e], mate)

        for k in range(NCH):
            res = product(k)
            for i in range(8):
                pbuf[k, i] = res[:, i * HD:(i + 1) * HD]
            pair_copy(k).start()
        if which == 0:
            flip(FLIPS[1])
        for k in range(NCH):
            pair_copy(k).wait_recv()
            for i in range(4):
                sbuf[k, i] = pbuf[k, core * 4 + i] + pair[k, i]
            for e in (2, 0, 1):
                scatter_copy(k, e).start()
        if which == 0:
            flip(FLIPS[2])
        for k in range(NCH):
            for e in range(3):
                scatter_copy(k, e).wait_recv()
            total = sbuf[k, quarter] + rs[k, 0] + rs[k, 1] + rs[k, 2]
            ag[k * 8 + own] = (base(k * 8 + own) + total).astype(BF16).astype(F32)
            for e in (2, 0, 1, 3):
                gather_copy(k, e).start()
        if which == 0:
            flip(FLIPS[3])
        for k in range(NCH):
            for e in range(3):
                gather_copy(k, e).wait_recv()
                forward_copy(k, e).start()
        if which == 0:
            flip(FLIPS[4])
            for block in range(sum(FLIPS) + AHEAD, len(order)):
                gate_copy(*order[block]).start()
        for k in range(NCH):
            gather_copy(k, 3).wait_recv()
            for e in range(3):
                forward_copy(k, e).wait_recv()
        for k in range(NCH):
            pair_copy(k).wait_send()
            for e in range(3):
                scatter_copy(k, e).wait_send()
                forward_copy(k, e).wait_send()
            for e in range(4):
                gather_copy(k, e).wait_send()

    def o_product(k):
        return jnp.dot(attn[...], wo[:, k * CW:(k + 1) * CW], preferred_element_type=F32)

    def x_base(i):
        return x_ref[:, pl.ds(pl.multiple_of(i * HD, HD), HD)].astype(F32)

    all_sum(0, o_product, x_base, pair_a, rs_a, ag_a)

    squares = jnp.zeros((B, HD), F32)
    for i in range(D // HD):
        squares = squares + ag_a[i] * ag_a[i]
    inv = lax.rsqrt(jnp.sum(squares, axis=-1, keepdims=True) / D + EPS)
    for i in range(D // HD):
        n_ref[:, i * HD:(i + 1) * HD] = (ag_a[i] * inv * g_ref[i:i + 1, :].astype(F32)).astype(BF16)

    def act(gate, up):
        return (jax.nn.silu(gate) * up).astype(BF16)

    for i, (first, n) in enumerate(spans):
        rows = pl.ds(first, n)
        for which in range(2):
            if 2 * i + which >= sum(FLIPS):
                gate_copy(i, which).wait()
        sums = [None, None]
        for k in range(D // GCH):
            cols = slice(k * GCH, (k + 1) * GCH)
            for which in range(2):
                dims = (((1,), (0 if 2 * i + which < sum(FLIPS) else 1,)), ((), ()))
                term = lax.dot_general(n_ref[:, cols], w2[which, rows, cols], dims, preferred_element_type=F32)
                sums[which] = term if k == 0 else sums[which] + term
        y_ref[:, first:first + n] = act(sums[0], sums[1])
        down_copy(i).start()
    for i in range(len(spans)):
        down_copy(i).wait()

    def down_product(k):
        return jnp.dot(y_ref[...], w2[0, :, k * CW:(k + 1) * CW], preferred_element_type=F32)

    all_sum(1, down_product, lambda i: ag_a[i], pair_b, rs_b, ag_b)
    for i in range(D // HD):
        out_ref[:, i * HD:(i + 1) * HD] = ag_b[i].astype(BF16)
    for d in (1, 2, 3):
        combine_copy(d).wait_send()


def vmem():
    return pl.BlockSpec(memory_space=pltpu.VMEM)


def hbm():
    return pl.BlockSpec(memory_space=pl.ANY)


def in_hbm(a):
    return pltpu.with_memory_space_constraint(a, pltpu.HBM)


def in_vmem(a):
    return pltpu.with_memory_space_constraint(a, pltpu.VMEM)


def smem():
    return pl.BlockSpec(memory_space=pltpu.SMEM)


def dma(*shape):
    return pltpu.SemaphoreType.DMA(shape)


def layer_step(x_in, ctx_len, g_attn, g_mlp, w_qkv, w_o, w_gate, w_up, w_down, k_cache, v_cache):
    freq = ROPE_THETA ** (-2.0 * np.arange(HD // 2, dtype=np.float64) / HD)
    freq = np.concatenate([freq, freq]).astype(np.float32).reshape(1, HD)
    kc = k_cache.reshape(B, T * KVL, HD)
    vc = v_cache.reshape(B, T * KVL, HD)
    nch = len(CHUNKS)
    q2, kn, vn, kv, vv = pl.pallas_call(
        qkv_kernel,
        out_shape=(pltpu.VMEM((B * ROWS, HD), F32), pltpu.VMEM((B * 8, HD), F32), pltpu.VMEM((B * 8, HD), F32),
                   pltpu.VMEM((B, CPITCH, HD), BF16), pltpu.VMEM((B, CPITCH, HD), BF16)),
        in_specs=[smem(), vmem(), hbm(), hbm(), hbm(), hbm(), hbm()],
        out_specs=(vmem(),) * 5,
        scratch_shapes=[
            pltpu.VMEM((B, D), BF16), pltpu.VMEM((D // HD, HD), BF16),
            pltpu.VMEM((D, QCOLS), BF16), pltpu.VMEM((B, D), BF16), pltpu.VMEM((KVL, GRP + 2, B, HD), F32),
            dma(2), dma(4 * WPARTS + 2 * CPARTS), dma(nch), dma(nch), dma(nch), dma(nch), dma(nch), dma(nch),
        ],
        compiler_params=pltpu.CompilerParams(collective_id=0, has_side_effects=True, vmem_limit_bytes=MIB * 16),
        name="qkv",
    )(in_hbm(ctx_len), in_hbm(freq), in_hbm(x_in), in_hbm(g_attn.reshape(D // HD, HD)), in_hbm(w_qkv), in_hbm(kc), in_hbm(vc))

    part, _, _, k_out, v_out = pl.pallas_call(
        attn_kernel,
        out_shape=(pltpu.VMEM((KVL, GRP + 1, B, HD), F32), pltpu.VMEM((B, CPITCH, HD), BF16), pltpu.VMEM((B, CPITCH, HD), BF16),
                   jax.ShapeDtypeStruct(kc.shape, BF16), jax.ShapeDtypeStruct(vc.shape, BF16)),
        in_specs=[smem(), vmem(), vmem(), vmem(), vmem(), vmem()],
        out_specs=(vmem(), vmem(), vmem(), hbm(), hbm()),
        scratch_shapes=[
            pltpu.VMEM((2 * ROWS, KVL * T), F32),
            pltpu.VMEM((B * ROWS, HD), F32), pltpu.VMEM((B * ROWS, HD), F32), pltpu.VMEM((B * ROWS, HD), F32),
            dma(2, B // 4),
        ],
        input_output_aliases={4: 1, 5: 2},
        compiler_params=pltpu.CompilerParams(vmem_limit_bytes=MIB * 4),
        name="attn",
    )(in_hbm(ctx_len), q2, kn, vn, kv, vv)

    x_out = pl.pallas_call(
        tail_kernel,
        out_shape=pltpu.VMEM((B, D), BF16),
        in_specs=[vmem(), hbm(), hbm(), hbm(), hbm(), hbm(), hbm()],
        out_specs=vmem(),
        scratch_shapes=[
            pltpu.VMEM((B, D), BF16), pltpu.VMEM((D // HD, HD), BF16), pltpu.VMEM(w_o.shape, BF16), pltpu.VMEM((2, FFL, D + HD), BF16),
            pltpu.VMEM((3, GRP + 1, B, HD), F32), pltpu.VMEM((B, GRP * HD), BF16), pltpu.VMEM((B, D), BF16), pltpu.VMEM((B, FFL), BF16),
            pltpu.VMEM((NCH, 8, B, HD), F32), pltpu.VMEM((NCH, 4, B, HD), F32),
            pltpu.VMEM((NCH, 4, B, HD), F32), pltpu.VMEM((NCH, 4, B, HD), F32),
            pltpu.VMEM((NCH, 3, B, HD), F32), pltpu.VMEM((NCH, 3, B, HD), F32),
            pltpu.VMEM((D // HD, B, HD), F32), pltpu.VMEM((D // HD, B, HD), F32),
            dma(2), pltpu.SemaphoreType.DMA, dma(2, 7), dma(7), dma(3), dma(3),
            dma(2, NCH), dma(2, NCH), dma(2, NCH, 3), dma(2, NCH, 3), dma(2, NCH, 4), dma(2, NCH, 4), dma(2, NCH, 3), dma(2, NCH, 3),
        ],
        compiler_params=pltpu.CompilerParams(collective_id=1, has_side_effects=True, vmem_limit_bytes=TAIL_VMEM),
        cost_estimate=pl.CostEstimate(flops=10 ** 10, bytes_accessed=10 ** 8, transcendentals=0),
        name="tail",
    )(in_vmem(part), in_hbm(x_in), in_hbm(g_mlp.reshape(D // HD, HD)), in_hbm(w_o), in_hbm(w_gate.T), in_hbm(w_up.T), in_hbm(w_down))
    return x_out, k_out.reshape(k_cache.shape), v_out.reshape(v_cache.shape)


def solution(mesh):
    x_spec = P("dp", None)
    cache_spec = P("dp", "kvp", "tp", None)
    model_axes = ("tp", "kvp")
    in_specs = (x_spec, P("dp"), P(None), P(None), P(None, "tp"), P(model_axes, None), P(None, model_axes), P(None, model_axes), P(model_axes, None), cache_spec, cache_spec)
    return jax.shard_map(layer_step, mesh=mesh, in_specs=in_specs, out_specs=(x_spec, cache_spec, cache_spec), check_vma=False)
```
